32 devices in a mesh: stream: 8 (over y, x, core), leaf: 4 (over z).
Axes of the slice: x: 2, y: 2, z: 4, core: 2. Of those that a mesh axis runs over, the one named last changes fastest.
Arguments:
- points_rhs: bfloat16 [2048, 32, 128], P(('stream', 'leaf')), may hold values from -6 to 6
- leaf_basis: bfloat16 [2048, 64, 128], P(('stream', 'leaf')), may hold values from -0.5 to 0.5
- transfer: bfloat16 [1024, 64, 128], P(('stream', 'leaf')), may hold values from -0.5 to 0.5
- leaf_coupling: bfloat16 [2048, 64, 256], P(('stream', 'leaf')), may hold values from -0.375 to 0.375
- parent_coupling: bfloat16 [1024, 64, 512], P(('stream', 'leaf')), may hold values from -0.25 to 0.25
- near_blocks: bfloat16 [2048, 3, 128, 128], P(('stream', 'leaf')), may hold values from -0.3125 to 0.3125
- near_offsets: int32 [2048, 3], P(('stream', 'leaf')), may hold values from -2 to 2, as said below
- coupling_offsets: int32 [2048, 4], P(('stream', 'leaf')), may hold values from -5 to 5, as said below
- parent_owner: int32 [1024, 8], P(('stream', 'leaf')), may hold values from 0 to 31, all different within a row; in each aligned block of 32 rows (0 to 31, 32 to 63, ...) at most 16 rows name the same one
- parent_local: int32 [1024, 8], P(('stream', 'leaf')), may hold values from 0 to 31
Outputs:
- product: bfloat16 [2048, 32, 128], P(('stream', 'leaf'))
The draws below stay inside these ranges and needn't reach their ends.
Inputs may be any that keep to these rules, and one draw needn't show every extreme that they name: `near_offsets`: each row holds 3 different offsets; the first is 0. `coupling_offsets`: each row holds 4 different nonzero offsets, none of which stands in the same row of near_offsets. `parent_owner`: each row names 8 different blocks; the rows of one device name no block more than 16 times, and in every draw some block is named exactly 16 times by the rows of some device.
All inputs are finite; a program needn't handle non-finite values.
Results may differ from the reference program's by a relative error of at most 0.0053.
Values may be sent and summed in bfloat16 or wider, within the bound.
A program may use at most 128 MiB of HBM per device.

```python
import math
import jax
import jax.numpy as jnp
import numpy as np
from jax import lax

R = 64
NRHS = 32
LS = 128
KN = 3
KC = 4
KP = 8
LEAF_DEV = 64
PAR_DEV = 32
NLEAF = 2048
NPAR = 1024
CAP = 16
DEVICES = 32


def leaf_lists(key):
    key_near = jax.random.fold_in(key, 11)
    key_far = jax.random.fold_in(key, 23)
    near_pool = jnp.array([-2, -1, 1, 2], jnp.int32)
    far_pool = jnp.array([-5, -4, -3, 3, 4, 5], jnp.int32)
    near_scores = jax.random.randint(key_near, (NLEAF, 4), 0, 1 << 20, dtype=jnp.int32) * 16 + jnp.arange(4, dtype=jnp.int32)
    near_order = jnp.argsort(near_scores, axis=1, stable=True)
    chosen = near_pool[near_order]
    near_rows = jnp.concatenate([jnp.zeros((NLEAF, 1), jnp.int32), chosen[:, :KN - 1]], axis=1)
    remaining = jnp.concatenate([chosen[:, KN - 1:], jnp.broadcast_to(far_pool, (NLEAF, 6))], axis=1)
    pool_size = 11 - KN
    far_scores = jax.random.randint(key_far, (NLEAF, pool_size), 0, 1 << 20, dtype=jnp.int32) * 16 + jnp.arange(pool_size, dtype=jnp.int32)
    far_order = jnp.argsort(far_scores, axis=1, stable=True)
    far_rows = jnp.take_along_axis(remaining, far_order, axis=1)[:, :KC]
    return (near_rows, far_rows)


def draw_near_offsets(key, part):
    return leaf_lists(key)[0]


def draw_coupling_offsets(key, part):
    return leaf_lists(key)[1]


def set_ends(entries, key, low, top_value):
    dims = entries.shape
    index_at = [jax.random.randint(jax.random.fold_in(key, axis), (), 0, dims[axis]) for axis in range(len(dims))]
    entries = entries.at[tuple(index_at)].set(low)
    longest = dims.index(max(dims))
    index_at[longest] = (index_at[longest] + 1) % dims[longest]
    return entries.at[tuple(index_at)].set(top_value)


def steps_of(stream_key, shape, pieces, smallest, largest):
    def one(dim, shards_of):
        draws = jax.random.uniform(jax.random.fold_in(jax.random.fold_in(stream_key, 6), dim), (shards_of,), jnp.float32, smallest / len(pieces), largest / len(pieces))
        return jnp.repeat(jnp.exp(draws), shape[dim] // shards_of).reshape((-1,) + (1,) * (len(shape) - dim - 1))

    level = one(*pieces[0])
    for cut in pieces[1:]:
        level = level * one(*cut)
    return level


def deal_out(own_key, own, number, rows, amount, top, bound, skew):
    sequence = jax.random.permutation(own_key, amount)
    crowded, usual = portions_of(amount, rows * top, bound, skew, True), portions_of(amount, rows * top, bound, skew, False)
    places = jnp.arange(amount)

    def named(sizes, turn):
        used = int((sizes > 0).sum())
        fixed = max(1, used // 4)
        moved = fixed + (places - fixed + turn * (used - fixed)) % max(1, amount - fixed)
        return jnp.zeros((amount,), jnp.int32).at[sequence[jnp.where(places < fixed, places, moved)]].set(jnp.asarray(sizes, jnp.int32))

    sizes = jnp.where(number % 4 == 0, named(crowded, number // 4), named(usual, number - number // 4 - 1))
    mixed = jax.random.permutation(jax.random.fold_in(own, 3), amount)
    source_of, taker = mixed[0:amount // 2 * 2:2], mixed[1:amount // 2 * 2:2]
    room = jnp.minimum(sizes[source_of] - 1, bound - sizes[taker]) // 2
    room = jnp.where((source_of == sequence[0]) | (taker == sequence[0]) | (sizes[taker] == 0), 0, jnp.maximum(room, 0))
    moved = jax.random.randint(jax.random.fold_in(own, 4), (amount // 2,), 0, 1 << 20) % (room + 1)
    sizes = sizes.at[source_of].add(-moved).at[taker].add(moved)
    labels = jnp.searchsorted(jnp.cumsum(sizes), jnp.arange(rows * top), side="right").astype(jnp.int32)
    listing = labels.reshape(top, rows).T
    listing = listing[jax.random.permutation(jax.random.fold_in(own, 1), rows)]
    turn = jax.random.randint(jax.random.fold_in(own, 2), (rows, 1), 0, top)
    return jnp.take_along_axis(listing, (jnp.arange(top)[None, :] + turn) % top, axis=1)


def portions_of(amount, total, most, lean, full):
    weights = [(1 << 20) // math.isqrt(rank ** lean) + 1 for rank in range(1, amount + 1)]
    largest = most if full else min(most, max(-(-total // amount), total * weights[0] // sum(weights)))
    least = 1 if total - largest >= amount - 1 else 0
    holding, rest = [largest] + [least] * (amount - 1), total - largest - least * (amount - 1)
    while rest > 0:
        movable = [i for i in range(1, amount) if holding[i] < largest] or [i for i in range(1, amount) if holding[i] < most]
        pool, left = sum([weights[i] for i in movable]), rest
        for i in movable:
            addition = min(most - holding[i], max(1, left * weights[i] // pool), rest)
            holding[i] = holding[i] + addition
            rest = rest - addition
    return np.array(holding)


def scatter_about(rng, shape, spread, reach, shards=(), kind=jnp.bfloat16):
    drawn = spread * jax.random.normal(rng, shape, jnp.float32)
    if shards:
        drawn = drawn * steps_of(rng, shape, shards, -0.22, 0.18)
    return jnp.clip(drawn, -reach, reach).astype(kind)


def setup_inputs(seed: int = 0) -> dict:
    key_list = jax.random.split(jax.random.key(seed), 11)
    points_rhs = scatter_about(key_list[0], (NLEAF, NRHS, LS), 1.0, 6.0, ((0, 32),))
    leaf_basis = scatter_about(key_list[1], (NLEAF, R, LS), LS ** -0.5, 0.5, ((0, 32),))
    transfer = scatter_about(key_list[2], (NPAR, R, 2 * R), (2 * R) ** -0.5, 0.5, ((0, 32),))
    leaf_coupling = scatter_about(key_list[3], (NLEAF, R, KC * R), (KC * R) ** -0.5, 0.375, ((0, 32),))
    parent_coupling = scatter_about(key_list[4], (NPAR, R, KP * R), (KP * R) ** -0.5, 0.25, ((0, 32),))
    near_blocks = scatter_about(key_list[5], (NLEAF, KN, LS, LS), (KN * LS) ** -0.5, 0.3125, ((0, 32),))
    near_offsets = draw_near_offsets(jax.random.fold_in(key_list[10], 71), 0)
    coupling_offsets = draw_coupling_offsets(jax.random.fold_in(key_list[10], 71), 0)
    parent_owner_keys = jax.random.split(jax.random.fold_in(key_list[8], 1), NPAR // PAR_DEV)
    parent_owner_turns = jax.random.permutation(jax.random.fold_in(key_list[8], 3), NPAR // PAR_DEV)
    parent_owner = jax.vmap(lambda own, number: deal_out(jax.random.fold_in(key_list[8], 2), own, number, PAR_DEV, DEVICES, KP, CAP, 1))(parent_owner_keys, parent_owner_turns).reshape((NPAR, KP))
    parent_local = set_ends(jax.random.randint(key_list[9], (NPAR, KP), 0, PAR_DEV), jax.random.fold_in(key_list[9], 1), 0, PAR_DEV - 1).astype(jnp.int32)
    return {"points_rhs": points_rhs, "leaf_basis": leaf_basis, "transfer": transfer, "leaf_coupling": leaf_coupling, "parent_coupling": parent_coupling, "near_blocks": near_blocks, "near_offsets": near_offsets, "coupling_offsets": coupling_offsets, "parent_owner": parent_owner, "parent_local": parent_local}


def shifted_rows(padded, offsets, reach_leaves):
    row_count = offsets.shape[0]
    row_base = jnp.arange(row_count, dtype=jnp.int32)[:, None] + reach_leaves
    return padded[(row_base + offsets).astype(jnp.int32)]


def near_block(paired):
    return jnp.einsum('cknj,ckqj->cnq', paired[0].astype(jnp.float32), paired[1].astype(jnp.float32))


def reference(points_rhs, leaf_basis, transfer, leaf_coupling, parent_coupling, near_blocks, near_offsets, coupling_offsets, parent_owner, parent_local):
    leaf_coeffs = jnp.einsum('cnp,crp->cnr', points_rhs.astype(jnp.float32), leaf_basis.astype(jnp.float32)).astype(jnp.bfloat16)
    paired = leaf_coeffs.reshape(NPAR, 2, NRHS, R).transpose(0, 2, 1, 3).reshape(NPAR, NRHS, 2 * R)
    parent_coeffs = jnp.einsum('pnk,prk->pnr', paired.astype(jnp.float32), transfer.astype(jnp.float32)).astype(jnp.bfloat16)
    coeff_padded = jnp.pad(leaf_coeffs, ((5, 5), (0, 0), (0, 0)))
    sources = shifted_rows(coeff_padded, coupling_offsets, 5)
    coupling_panel = leaf_coupling.reshape(NLEAF, R, KC, R)
    leaf_field = jnp.einsum('cknj,crkj->cnr', sources.astype(jnp.float32), coupling_panel.astype(jnp.float32))
    source_rows = (parent_owner * PAR_DEV + parent_local).astype(jnp.int32)
    remote = parent_coeffs[source_rows]
    parent_panel = parent_coupling.reshape(NPAR, R, KP, R)
    parent_field = jnp.einsum('pknj,prkj->pnr', remote.astype(jnp.float32), parent_panel.astype(jnp.float32))
    parent_half = lax.optimization_barrier(parent_field.astype(jnp.bfloat16))
    downward = jnp.einsum('pnr,prk->pnk', parent_half.astype(jnp.float32), transfer.astype(jnp.float32))
    downward = downward.reshape(NPAR, NRHS, 2, R).transpose(0, 2, 1, 3).reshape(NLEAF, NRHS, R)
    leaf_total = (leaf_field + downward).astype(jnp.bfloat16)
    far_terms = jnp.einsum('cnr,crp->cnp', leaf_total.astype(jnp.float32), leaf_basis.astype(jnp.float32))
    point_padded = jnp.pad(points_rhs, ((2, 2), (0, 0), (0, 0)))
    near_rows = shifted_rows(point_padded, near_offsets, 2).reshape(DEVICES, LEAF_DEV, KN, NRHS, LS)
    block_rows = near_blocks.reshape(DEVICES, LEAF_DEV, KN, LS, LS)
    near_terms = lax.map(near_block, (near_rows, block_rows)).reshape(NLEAF, NRHS, LS)
    return (far_terms + near_terms).astype(jnp.bfloat16)
```

```python
import functools

import jax
import jax.numpy as jnp
from jax import lax
from jax.experimental import pallas as pl
from jax.experimental.pallas import tpu as pltpu
from jax.sharding import PartitionSpec as P

NEAR_REACH = 2
FAR_REACH = 5
MESH = pl.DeviceIdType.MESH
NT = (((1,), (1,)), ((), ()))
NN = (((1,), (0,)), ((), ()))


WIDTH = 8
PARTS = 4
CLOCK, NEAR_TIME, FAR_TIME = 1.0, 0.8, 0.4
READY_TIME, EDGE_TIME = 7.0, 12.0
WINDOWS = {
    (0, 1): (2.3, 4.8),
    (1, 0): (2.3, 4.8),
    (2, 0): (2.3, 4.8),
    (0, 2): (3.5, 6.0),
    (3, 0): (5.0, 7.5),
    (0, 3): (6.0, 9.0),
    (1, 2): (7.5, 10.5),
    (2, 2): (7.5, 10.5),
    (1, 1): (10.0, 14.0),
    (2, 1): (13.0, 16.0),
    (1, 3): (10.0, 13.5),
    (2, 3): (10.0, 13.5),
    (3, 2): (10.0, 13.0),
    (3, 1): (13.0, 17.0),
    (3, 3): (13.0, 17.0),
}
LATE = {1: (8.5, 10.5), 2: (10.5, 12.5)}


def line_order(line):
    table = [sorted(range(line), key=lambda other: ((other // 2 != z // 2) + (other != z), abs(other - z), other))
             for z in range(line)]
    for z in range(line):
        for other in range(line):
            if abs(other - z) > 1:
                nearer = z + (1 if other > z else -1)
                assert table[nearer].index(other) <= table[z].index(other)
    return table


def sends_of(line, nbits):
    sends = nbits + 3
    for step in range(line):
        for mask in range(1 << nbits):
            if mask or step:
                sends += 1 + (mask == 0)
                sends += 2 * bool(mask and mask & (mask - 1) == 0 and step == 0)
                sends += 0 if mask == 0 and step == 1 else nbits - mask.bit_length()
    return sends


def dot(a, b, dims):
    return lax.dot_general(a, b, dims, preferred_element_type=jnp.float32)


def bits_of(count):
    bits = count.bit_length() - 1
    assert 1 << bits == count
    return bits


def kernel(
    streams, line, parts,
    near_off_hbm, far_off_hbm, owner_hbm, local_hbm,
    points_hbm, basis_hbm, transfer_hbm, leaf_hbm, parent_hbm, near_hbm,
    out_hbm,
    near_off, far_off, owner, local,
    points, points_low, points_high, basis, transfer, leaf_panel, parent_panel, near_blocks,
    coeffs, coeffs_low, coeffs_high, gathered, near_sum, leaf_sum, out,
    index_sem, load_sem, edge_sem, near_sem, panel_sem, out_sem,
    halo_send, halo_recv, send_sem, recv_sem, ready,
):
    leaves, rhs, size = points_hbm.shape
    parents, rank, _ = transfer_hbm.shape
    kn = near_off.shape[0]
    kc = far_off.shape[0]
    kp = owner.shape[0]
    half = rhs // 2
    width = WIDTH
    groups = parents // width
    near_edge = points_low.shape[0] - NEAR_REACH
    far_edge = coeffs_low.shape[0] - FAR_REACH
    chunk = parents // parts
    nbits = bits_of(streams // 2)
    bits_of(line)
    assert line > 1
    near_parts = near_sem.shape[0]
    out_parts = out_sem.shape[0]

    my_s = lax.axis_index("stream")
    my_z = lax.axis_index("leaf")
    core = my_s % 2
    place = my_s // 2
    total_blocks = streams * line
    me = my_s * line + my_z

    def device(block):
        return (block // line, block % line)

    def block_of(h, z):
        return (h * 2 + core) * line + z

    def bit_at(phase):
        first = 1 << phase
        if nbits < 2:
            return first
        second = 1 << ((phase + 1) % nbits)
        return first + core * (second - first)

    def flip(h, bit):
        return h + bit * (1 - 2 * ((h // bit) % 2))

    def subset(mask):
        h = place
        for phase in range(nbits):
            if mask >> phase & 1:
                h = flip(h, bit_at(phase))
        return h

    table = line_order(line)
    planes = [my_z]
    for step in range(1, line):
        z = table[0][step]
        for row in range(1, line):
            z = jnp.where(my_z == row, table[row][step], z)
        planes.append(z)
    pair_z = flip(my_z, 1)
    cross_z = 2 * my_z - pair_z
    crosses = (cross_z >= 0) & (cross_z < line)
    cross_z = jnp.clip(cross_z, 0, line - 1)

    partners = [(flip(place, bit_at(i)) * 2 + core, my_z) for i in range(nbits)]
    pair = (my_s, pair_z)
    cross = (my_s, cross_z)
    sibling = (my_s + 1 - 2 * core, my_z)
    after = device((me + 1) % total_blocks)
    before = device((me + total_blocks - 1) % total_blocks)
    starts_line = my_z == 0
    ends_line = my_z == line - 1

    indices = [
        pltpu.make_async_copy(source, target, index_sem.at[i])
        for i, (source, target) in enumerate([
            (near_off_hbm, near_off), (far_off_hbm, far_off),
            (owner_hbm, owner), (local_hbm, local)])
    ]
    loads = [
        [pltpu.make_async_copy(source.at[pl.ds(g * step, step)],
                               target.at[pl.ds(g * step, step)], load_sem.at[3 * g + i])
         for i, (source, target, step) in enumerate([
             (points_hbm, points, 2 * width), (basis_hbm, basis, 2 * width),
             (transfer_hbm, transfer, width)])]
        for g in range(groups)
    ]
    edges = [
        pltpu.make_async_copy(points_hbm.at[pl.ds(0, near_edge)],
                              points_low.at[pl.ds(NEAR_REACH, near_edge)], edge_sem.at[0]),
        pltpu.make_async_copy(points_hbm.at[pl.ds(leaves - near_edge, near_edge)],
                              points_high.at[pl.ds(0, near_edge)], edge_sem.at[1]),
    ]
    panels = [
        pltpu.make_async_copy(leaf_hbm, leaf_panel, panel_sem.at[0]),
        pltpu.make_async_copy(parent_hbm, parent_panel, panel_sem.at[1]),
    ]
    near_rows = leaves // near_parts
    near_loads = [
        pltpu.make_async_copy(
            near_hbm.at[pl.ds(i * near_rows, near_rows)],
            near_blocks.at[pl.ds(i * near_rows, near_rows)],
            near_sem.at[i],
        )
        for i in range(near_parts)
    ]
    barrier = pltpu.get_barrier_semaphore()
    for load in loads[0]:
        load.start()
    greeted = partners + [pair, sibling]
    for other in greeted:
        pl.semaphore_signal(barrier, inc=1, device_id=other, device_id_type=MESH)

    @pl.when(crosses)
    def _():
        pl.semaphore_signal(barrier, inc=1, device_id=cross, device_id_type=MESH)

    @pl.when(starts_line)
    def _():
        pl.semaphore_signal(barrier, inc=1, device_id=before, device_id_type=MESH)

    for group in loads[1:]:
        for load in group:
            load.start()
    for load in indices + edges + near_loads + panels:
        load.start()

    low_lanes = lax.broadcasted_iota(jnp.int32, (rhs, 2 * rank), 1) < rank

    def upward(group):
        ps = [group * width + i for i in range(width)]
        boths = []
        for p in ps:
            pair = jnp.concatenate([points[2 * p], points[2 * p + 1]], axis=0)
            weights = basis[pl.ds(2 * p, 2)].reshape(2 * rank, size)
            boths.append(dot(pair, weights, NT))
        sides = [jnp.where(low_lanes, both[:rhs], both[rhs:]) for both in boths]
        ups = [dot(side.astype(jnp.bfloat16), transfer[p], NT) for p, side in zip(ps, sides)]
        for p, up in zip(ps, ups):
            packed = jnp.concatenate([up[:half], up[half:]], axis=1)
            gathered[me * parents + p] = packed.astype(jnp.bfloat16)
        for p, side in zip(ps, sides):
            rolled = pltpu.roll(side, rank, 1)
            for c, value in ((2 * p, jnp.where(low_lanes, side, rolled).astype(jnp.bfloat16)),
                             (2 * p + 1, jnp.where(low_lanes, rolled, side).astype(jnp.bfloat16))):
                coeffs[c] = value
                if c < far_edge:
                    coeffs_low[FAR_REACH + c] = value
                if c >= leaves - far_edge:
                    coeffs_high[c - (leaves - far_edge)] = value

    def halo(index, source, target, whom):
        return pltpu.make_async_remote_copy(
            src_ref=source, dst_ref=target,
            send_sem=halo_send.at[index], recv_sem=halo_recv.at[index],
            device_id=whom, device_id_type=MESH,
        )

    point_halos = [
        halo(0, points.at[pl.ds(leaves - NEAR_REACH, NEAR_REACH)],
             points_low.at[pl.ds(0, NEAR_REACH)], after),
        halo(1, points.at[pl.ds(0, NEAR_REACH)],
             points_high.at[pl.ds(near_edge, NEAR_REACH)], before),
    ]
    coeff_halos = [
        halo(2, coeffs.at[pl.ds(leaves - FAR_REACH, FAR_REACH)],
             coeffs_low.at[pl.ds(0, FAR_REACH)], after),
        halo(3, coeffs.at[pl.ds(0, FAR_REACH)],
             coeffs_high.at[pl.ds(far_edge, FAR_REACH)], before),
    ]

    sends = []

    def when(condition, action):
        if condition is None:
            action()
        else:
            pl.when(condition)(action)

    def span(block, part):
        return gathered.at[pl.ds(block * parents + part * chunk, chunk)]

    def send(block, part, whom, condition=None):
        copy = pltpu.make_async_remote_copy(
            src_ref=span(block, part), dst_ref=span(block, part),
            send_sem=send_sem.at[len(sends)], recv_sem=recv_sem.at[block * parts + part],
            device_id=whom, device_id_type=MESH,
        )
        when(condition, copy.start)
        sends.append((condition, copy))

    def arrived(block, part):
        pltpu.make_async_remote_copy(
            src_ref=span(block, part), dst_ref=span(block, part),
            send_sem=send_sem.at[0], recv_sem=recv_sem.at[block * parts + part],
            device_id=sibling, device_id_type=MESH,
        ).wait_recv()

    per_part = groups // parts
    for part in range(parts):
        for group in range(part * per_part, (part + 1) * per_part):
            for load in loads[group]:
                load.wait()
            upward(group)
        if part == 0:
            pl.semaphore_wait(barrier, len(greeted) + crosses.astype(jnp.int32) + ends_line.astype(jnp.int32))

            @pl.when(ends_line)
            def _():
                pl.semaphore_signal(ready, inc=1, device_id=after, device_id_type=MESH)

        send(me, part, pair)
        send(me, part, cross, crosses)
        for whom in partners + [sibling]:
            send(me, part, whom)

    for copy in (point_halos[0], coeff_halos[0]):
        copy.start()

    def send_back():
        for copy in (point_halos[1], coeff_halos[1]):
            copy.start()

    @pl.when(jnp.logical_not(starts_line))
    def _():
        send_back()

    def single(mask):
        return mask and mask & (mask - 1) == 0

    def relay(mask, step, part):
        block = block_of(subset(mask), planes[step])
        arrived(block, part)
        if mask == 0:
            onward = 2 * (planes[step] < my_z).astype(jnp.int32) - 1
            z = my_z + onward
            send(block, part, (my_s, jnp.clip(z, 0, line - 1)), (z >= 0) & (z < line))
        if single(mask) and step == 0:
            send(block, part, pair, jnp.logical_not(crosses))
        if not (mask == 0 and step == 1):
            for phase in range(mask.bit_length(), nbits):
                send(block, part, partners[phase])
        send(block, part, sibling)

    def relay_late(mask, step, part):
        send(block_of(subset(mask), planes[step]), part, pair, crosses)

    def window(mask, step):
        bits = bin(mask).count("1")
        if nbits == 2 and line == 4:
            return WINDOWS[(mask, step)]
        begin = 4 * bits + 3 * step
        return (begin, begin + 3.0)

    events = []
    for step in range(line):
        for mask in range(1 << nbits):
            if mask or step:
                spans = [(relay, window(mask, step))]
                if single(mask) and step == 0:
                    late = 6 if mask.bit_length() < nbits else 9
                    spans.append((relay_late, LATE[mask] if nbits == 2 and line == 4 else (late, late + 3.0)))
                for action, (begin, end) in spans:
                    for part in range(parts):
                        time = begin + (end - begin) * (part + 1) / parts
                        events.append((time, len(events), functools.partial(action, mask, step, part)))

    def send_back_late():
        @pl.when(starts_line)
        def _():
            pl.semaphore_wait(ready, 1)
            send_back()

    events.append((READY_TIME, len(events), send_back_late))
    events.sort()

    clock = [CLOCK]

    def advance(time):
        clock[0] += time
        while events and events[0][0] <= clock[0]:
            events.pop(0)[2]()

    first = me == 0
    last = me == total_blocks - 1

    def near(group, rows_of, shift):
        cs = [group * width + i for i in range(width)]
        sums = []
        for c in cs:
            rows = [rows_of[c + shift + near_off[k, c]] for k in range(kn)]
            weights = [near_blocks[c, k] for k in range(kn)]
            sums.append(dot(jnp.concatenate(rows, axis=1), jnp.concatenate(weights, axis=1), NT))
        for c, value in zip(cs, sums):
            near_sum[c] = value

    def one_leaf(c, rows_of, shift):
        rows = [rows_of[c + shift + far_off[k, c]] for k in range(kc)]
        sides = [jnp.where(low_lanes, rows[k], rows[k + 1]) for k in range(0, kc, 2)]
        return dot(jnp.concatenate(sides, axis=1), leaf_panel[c], NT)

    def coupling(group, rows_of, shift):
        ps = [group * (width // 2) + i for i in range(width // 2)]
        pairs = [(one_leaf(2 * p, rows_of, shift), one_leaf(2 * p + 1, rows_of, shift)) for p in ps]
        for p, pair in zip(ps, pairs):
            leaf_sum[p] = jnp.concatenate(pair, axis=1)

    leaf_groups = leaves // width
    inner = list(range(1, leaf_groups - 1))
    for copy in indices:
        copy.wait()
    loaded = set()

    def near_piece(group, rows_of, shift):
        part = group * width // near_rows
        if part not in loaded:
            near_loads[part].wait()
            loaded.add(part)
        near(group, rows_of, shift)
        advance(NEAR_TIME)

    for group in inner:
        near_piece(group, points, 0)
    panels[0].wait()
    for group in inner:
        coupling(group, coeffs, 0)
        advance(FAR_TIME)

    advance(EDGE_TIME - clock[0])
    for copy in edges + point_halos + coeff_halos:
        copy.wait()

    @pl.when(first)
    def _():
        points_low[pl.ds(0, NEAR_REACH)] = jnp.zeros((NEAR_REACH, rhs, size), jnp.bfloat16)
        coeffs_low[pl.ds(0, FAR_REACH)] = jnp.zeros((FAR_REACH, rhs, 2 * rank), jnp.bfloat16)

    @pl.when(last)
    def _():
        points_high[pl.ds(near_edge, NEAR_REACH)] = jnp.zeros((NEAR_REACH, rhs, size), jnp.bfloat16)
        coeffs_high[pl.ds(far_edge, FAR_REACH)] = jnp.zeros((FAR_REACH, rhs, 2 * rank), jnp.bfloat16)

    near_piece(0, points_low, NEAR_REACH)
    near_piece(leaf_groups - 1, points_high, near_edge - leaves)
    coupling(0, coeffs_low, FAR_REACH)
    advance(FAR_TIME)
    coupling(leaf_groups - 1, coeffs_high, far_edge - leaves)
    advance(1e9)

    for h in range(1 << nbits):
        for z in range(line):
            for part in range(parts):
                arrived((h * 2 + 1 - core) * line + z, part)
    panels[1].wait()

    low_half = lax.broadcasted_iota(jnp.int32, (half, 2 * rank), 1) < rank

    def remote_rows(p):
        tiles = [gathered[owner[k, p] * parents + local[k, p]] for k in range(kp)]
        upper, lower = [], []
        for k in range(0, kp, 2):
            a, b = tiles[k], tiles[k + 1]
            turned_a = jnp.concatenate([a[:, rank:], a[:, :rank]], axis=1)
            turned_b = jnp.concatenate([b[:, rank:], b[:, :rank]], axis=1)
            upper.append(jnp.where(low_half, a, turned_b))
            lower.append(jnp.where(low_half, turned_a, b))
        return jnp.concatenate(
            [jnp.concatenate(upper, axis=1), jnp.concatenate(lower, axis=1)], axis=0)

    def downward(group, _):
        ps = [group * width + i for i in range(width)]
        fields = [dot(remote_rows(p), parent_panel[p], NT).astype(jnp.bfloat16) for p in ps]
        totals = [leaf_sum[p] + dot(field, transfer[p], NN) for p, field in zip(ps, fields)]
        fars = []
        for p, total in zip(ps, totals):
            zero = jnp.zeros_like(total)
            stacked = jnp.concatenate(
                [jnp.where(low_lanes, total, zero), jnp.where(low_lanes, zero, total)], axis=0)
            weights = basis[pl.ds(2 * p, 2)].reshape(2 * rank, size)
            fars.append(dot(stacked.astype(jnp.bfloat16), weights, NN))
        for p, far in zip(ps, fars):
            out[2 * p] = (far[:rhs] + near_sum[2 * p]).astype(jnp.bfloat16)
            out[2 * p + 1] = (far[rhs:] + near_sum[2 * p + 1]).astype(jnp.bfloat16)
        return 0

    stores = []
    per_part = groups // out_parts
    for part in range(out_parts):
        lax.fori_loop(part * per_part, (part + 1) * per_part, downward, 0)
        rows = pl.ds(2 * part * per_part * width, 2 * per_part * width)
        stores.append(pltpu.make_async_copy(out.at[rows], out_hbm.at[rows], out_sem.at[part]))
        stores[-1].start()
    for condition, copy in sends:
        when(condition, copy.wait_send)
    for copy in stores:
        copy.wait()


def on_device(
    streams,
    line,
    points_rhs,
    leaf_basis,
    transfer,
    leaf_coupling,
    parent_coupling,
    near_blocks,
    near_offsets,
    coupling_offsets,
    parent_owner,
    parent_local,
):
    leaves, rhs, size = points_rhs.shape
    parents, rank, _ = transfer.shape
    places = streams // 2
    nbits = bits_of(places)
    blocks = streams * line
    parts, near_parts, out_parts = PARTS, 4, 4
    copies = sends_of(line, nbits) * parts
    hbm = pl.BlockSpec(memory_space=pl.ANY)
    bf16 = jnp.bfloat16
    dma = pltpu.SemaphoreType.DMA
    near_edge, far_edge = WIDTH + NEAR_REACH, WIDTH + FAR_REACH
    groups = parents // WIDTH
    offsets = [x.T for x in (near_offsets, coupling_offsets, parent_owner, parent_local)]
    return pl.pallas_call(
        functools.partial(kernel, streams, line, parts),
        out_shape=jax.ShapeDtypeStruct(points_rhs.shape, bf16),
        in_specs=[hbm] * 10,
        out_specs=hbm,
        scratch_shapes=[
            *[pltpu.SMEM(x.shape, jnp.int32) for x in offsets],
            pltpu.VMEM(points_rhs.shape, bf16),
            pltpu.VMEM((near_edge + NEAR_REACH, rhs, size), bf16),
            pltpu.VMEM((near_edge + NEAR_REACH, rhs, size), bf16),
            pltpu.VMEM(leaf_basis.shape, bf16),
            pltpu.VMEM(transfer.shape, bf16),
            pltpu.VMEM(leaf_coupling.shape, bf16),
            pltpu.VMEM(parent_coupling.shape, bf16),
            pltpu.VMEM(near_blocks.shape, bf16),
            pltpu.VMEM((leaves, rhs, 2 * rank), bf16),
            pltpu.VMEM((far_edge + FAR_REACH, rhs, 2 * rank), bf16),
            pltpu.VMEM((far_edge + FAR_REACH, rhs, 2 * rank), bf16),
            pltpu.VMEM((blocks * parents, rhs // 2, 2 * rank), bf16),
            pltpu.VMEM((leaves, rhs, size), jnp.float32),
            pltpu.VMEM((parents, rhs, 2 * rank), jnp.float32),
            pltpu.VMEM((leaves, rhs, size), bf16),
            dma((4,)),
            dma((3 * groups,)),
            dma((2,)),
            dma((near_parts,)),
            dma((2,)),
            dma((out_parts,)),
            dma((4,)),
            dma((4,)),
            dma((copies,)),
            dma((blocks * parts,)),
            pltpu.SemaphoreType.REGULAR,
        ],
        compiler_params=pltpu.CompilerParams(collective_id=0, has_side_effects=True),
    )(
        *offsets,
        points_rhs, leaf_basis, transfer, leaf_coupling, parent_coupling, near_blocks,
    )


def solution(mesh):
    whole = P(("stream", "leaf"))
    return jax.shard_map(
        functools.partial(on_device, mesh.shape["stream"], mesh.shape["leaf"]),
        mesh=mesh,
        in_specs=(whole,) * 10,
        out_specs=whole,
        check_vma=False,
    )
```

```python
import functools

import jax
import jax.numpy as jnp
from jax import lax
from jax.experimental import pallas as pl
from jax.experimental.pallas import tpu as pltpu
from jax.sharding import PartitionSpec as P

NEAR_REACH = 2
FAR_REACH = 5
MESH = pl.DeviceIdType.MESH
NT = (((1,), (1,)), ((), ()))
NN = (((1,), (0,)), ((), ()))


WIDTH = 8
VMEM_LIMIT = 40 << 20
PARTS = 4
CLOCK, NEAR_TIME, FAR_TIME = 1.0, 0.8, 0.4
READY_TIME, EDGE_TIME = 4.4, 14.2
MIDDLE = {
    (0, 1): (1.2, 4.0),
    (1, 0): (2.3, 4.8),
    (2, 0): (2.3, 4.8),
    (0, 2): (0.6, 2.8),
    (0, 3): (4.0, 8.0),
    (1, 2): (5.0, 9.0),
    (2, 2): (9.5, 11.0),
    (1, 1): (11.0, 13.0),
    (1, 3): (11.0, 13.0),
    (2, 1): (13.0, 14.0),
    (2, 3): (12.5, 14.0),
    (3, 0): (13.9, 14.1),
    (3, 2): (14.4, 15.0),
    (3, 1): (15.0, 17.0),
    (3, 3): (15.5, 17.5),
}
END = {
    (0, 1): (2.3, 4.8),
    (1, 0): (2.3, 4.8),
    (2, 0): (2.3, 4.8),
    (0, 2): (3.5, 6.0),
    (0, 3): (6.0, 9.0),
    (1, 2): (9.5, 11.0),
    (2, 2): (9.5, 11.0),
    (1, 1): (11.0, 13.0),
    (1, 3): (11.0, 13.0),
    (2, 1): (13.0, 14.0),
    (2, 3): (12.5, 14.0),
    (3, 0): (13.9, 14.1),
    (3, 2): (14.4, 15.0),
    (3, 1): (15.0, 17.0),
    (3, 3): (15.5, 17.5),
}
LATE = {1: (8.2, 8.6), 2: (9.0, 10.0)}


def line_order(line):
    table = [sorted(range(line), key=lambda other: ((other // 2 != z // 2) + (other != z), abs(other - z), other))
             for z in range(line)]
    for z in range(line):
        for other in range(line):
            if abs(other - z) > 1:
                nearer = z + (1 if other > z else -1)
                assert table[nearer].index(other) <= table[z].index(other)
    return table


def sends_of(line, nbits):
    sends = nbits + 3
    for step in range(line):
        for mask in range(1 << nbits):
            if mask or step:
                sends += 1 + (mask == 0)
                sends += 2 * bool(mask and mask & (mask - 1) == 0 and step == 0)
                sends += 0 if mask == 0 and step == 1 else nbits - mask.bit_length()
    return sends


def dot(a, b, dims):
    return lax.dot_general(a, b, dims, preferred_element_type=jnp.float32)


def bits_of(count):
    bits = count.bit_length() - 1
    assert 1 << bits == count
    return bits


def kernel(
    streams, line, parts,
    near_off_hbm, far_off_hbm, owner_hbm, local_hbm,
    points_hbm, basis_hbm, transfer_hbm, leaf_hbm, parent_hbm, near_hbm,
    out,
    near_off, far_off, owner, local,
    points, points_low, points_high, basis, transfer, leaf_panel, parent_panel, near_blocks,
    coeffs, coeffs_low, coeffs_high, gathered, near_sum, leaf_sum,
    index_sem, load_sem, edge_sem, near_sem, panel_sem,
    halo_send, halo_recv, send_sem, recv_sem, ready,
):
    leaves, rhs, size = points_hbm.shape
    parents, rank, _ = transfer_hbm.shape
    kn = near_off.shape[0]
    kc = far_off.shape[0]
    kp = owner.shape[0]
    half = rhs // 2
    width = WIDTH
    groups = parents // width
    near_edge = points_low.shape[0] - NEAR_REACH
    far_edge = coeffs_low.shape[0] - FAR_REACH
    chunk = parents // parts
    nbits = bits_of(streams // 2)
    bits_of(line)
    assert line > 1
    near_parts = near_sem.shape[0]

    my_s = lax.axis_index("stream")
    my_z = lax.axis_index("leaf")
    core = my_s % 2
    place = my_s // 2
    total_blocks = streams * line
    me = my_s * line + my_z

    def device(block):
        return (block // line, block % line)

    def block_of(h, z):
        return (h * 2 + core) * line + z

    def bit_at(phase):
        first = 1 << phase
        if nbits < 2:
            return first
        second = 1 << ((phase + 1) % nbits)
        return first + core * (second - first)

    def flip(h, bit):
        return h + bit * (1 - 2 * ((h // bit) % 2))

    def subset(mask):
        h = place
        for phase in range(nbits):
            if mask >> phase & 1:
                h = flip(h, bit_at(phase))
        return h

    table = line_order(line)
    planes = [my_z]
    for step in range(1, line):
        z = table[0][step]
        for row in range(1, line):
            z = jnp.where(my_z == row, table[row][step], z)
        planes.append(z)
    pair_z = flip(my_z, 1)
    cross_z = 2 * my_z - pair_z
    crosses = (cross_z >= 0) & (cross_z < line)
    cross_z = jnp.clip(cross_z, 0, line - 1)

    partners = [(flip(place, bit_at(i)) * 2 + core, my_z) for i in range(nbits)]
    pair = (my_s, pair_z)
    cross = (my_s, cross_z)
    sibling = (my_s + 1 - 2 * core, my_z)
    after = device((me + 1) % total_blocks)
    before = device((me + total_blocks - 1) % total_blocks)
    starts_line = my_z == 0
    ends_line = my_z == line - 1

    indices = [
        pltpu.make_async_copy(source, target, index_sem.at[i])
        for i, (source, target) in enumerate([
            (near_off_hbm, near_off), (far_off_hbm, far_off),
            (owner_hbm, owner), (local_hbm, local)])
    ]
    loads = [
        [pltpu.make_async_copy(source.at[pl.ds(g * step, step)],
                               target.at[pl.ds(g * step, step)], load_sem.at[3 * g + i])
         for i, (source, target, step) in enumerate([
             (points_hbm, points, 2 * width), (basis_hbm, basis, 2 * width),
             (transfer_hbm, transfer, width)])]
        for g in range(groups)
    ]
    edges = [
        pltpu.make_async_copy(points_hbm.at[pl.ds(0, near_edge)],
                              points_low.at[pl.ds(NEAR_REACH, near_edge)], edge_sem.at[0]),
        pltpu.make_async_copy(points_hbm.at[pl.ds(leaves - near_edge, near_edge)],
                              points_high.at[pl.ds(0, near_edge)], edge_sem.at[1]),
    ]
    panels = [
        pltpu.make_async_copy(leaf_hbm, leaf_panel, panel_sem.at[0]),
        pltpu.make_async_copy(parent_hbm, parent_panel, panel_sem.at[1]),
    ]
    near_rows = leaves // near_parts
    near_loads = [
        pltpu.make_async_copy(
            near_hbm.at[pl.ds(i * near_rows, near_rows)],
            near_blocks.at[pl.ds(i * near_rows, near_rows)],
            near_sem.at[i],
        )
        for i in range(near_parts)
    ]
    barrier = pltpu.get_barrier_semaphore()
    for load in loads[0]:
        load.start()
    greeted = partners + [pair, sibling]
    for other in greeted:
        pl.semaphore_signal(barrier, inc=1, device_id=other, device_id_type=MESH)

    @pl.when(crosses)
    def _():
        pl.semaphore_signal(barrier, inc=1, device_id=cross, device_id_type=MESH)

    @pl.when(starts_line)
    def _():
        pl.semaphore_signal(barrier, inc=1, device_id=before, device_id_type=MESH)

    for group in loads[1:]:
        for load in group:
            load.start()
    for load in indices + edges + near_loads + panels:
        load.start()

    low_lanes = lax.broadcasted_iota(jnp.int32, (rhs, 2 * rank), 1) < rank

    def upward(group):
        ps = [group * width + i for i in range(width)]
        boths = []
        for p in ps:
            pair = jnp.concatenate([points[2 * p], points[2 * p + 1]], axis=0)
            weights = basis[pl.ds(2 * p, 2)].reshape(2 * rank, size)
            boths.append(dot(pair, weights, NT))
        sides = [jnp.where(low_lanes, both[:rhs], both[rhs:]) for both in boths]
        ups = [dot(side.astype(jnp.bfloat16), transfer[p], NT) for p, side in zip(ps, sides)]
        for p, up in zip(ps, ups):
            packed = jnp.concatenate([up[:half], up[half:]], axis=1)
            gathered[me * parents + p] = packed.astype(jnp.bfloat16)
        for p, side in zip(ps, sides):
            rolled = pltpu.roll(side, rank, 1)
            for c, value in ((2 * p, jnp.where(low_lanes, side, rolled).astype(jnp.bfloat16)),
                             (2 * p + 1, jnp.where(low_lanes, rolled, side).astype(jnp.bfloat16))):
                coeffs[c] = value
                if c < far_edge:
                    coeffs_low[FAR_REACH + c] = value
                if c >= leaves - far_edge:
                    coeffs_high[c - (leaves - far_edge)] = value

    def halo(index, source, target, whom):
        return pltpu.make_async_remote_copy(
            src_ref=source, dst_ref=target,
            send_sem=halo_send.at[index], recv_sem=halo_recv.at[index],
            device_id=whom, device_id_type=MESH,
        )

    point_halos = [
        halo(0, points.at[pl.ds(leaves - NEAR_REACH, NEAR_REACH)],
             points_low.at[pl.ds(0, NEAR_REACH)], after),
        halo(1, points.at[pl.ds(0, NEAR_REACH)],
             points_high.at[pl.ds(near_edge, NEAR_REACH)], before),
    ]
    coeff_halos = [
        halo(2, coeffs.at[pl.ds(leaves - FAR_REACH, FAR_REACH)],
             coeffs_low.at[pl.ds(0, FAR_REACH)], after),
        halo(3, coeffs.at[pl.ds(0, FAR_REACH)],
             coeffs_high.at[pl.ds(far_edge, FAR_REACH)], before),
    ]

    sends = {}

    def when(condition, action):
        if condition is None:
            action()
        else:
            pl.when(condition)(action)

    def span(block, part):
        return gathered.at[pl.ds(block * parents + part * chunk, chunk)]

    def send(name, block, part, whom, condition=None):
        index, _ = sends.setdefault((name, part), (len(sends), condition))
        when(condition, pltpu.make_async_remote_copy(
            src_ref=span(block, part), dst_ref=span(block, part),
            send_sem=send_sem.at[index], recv_sem=recv_sem.at[block * parts + part],
            device_id=whom, device_id_type=MESH,
        ).start)

    def sent(index):
        pltpu.make_async_remote_copy(
            src_ref=span(me, 0), dst_ref=span(me, 0), send_sem=send_sem.at[index], recv_sem=recv_sem.at[0],
            device_id=sibling, device_id_type=MESH,
        ).wait_send()

    def arrived(block, part):
        pltpu.make_async_remote_copy(
            src_ref=span(block, part), dst_ref=span(block, part),
            send_sem=send_sem.at[0], recv_sem=recv_sem.at[block * parts + part],
            device_id=sibling, device_id_type=MESH,
        ).wait_recv()

    per_part = groups // parts
    for part in range(parts):
        for group in range(part * per_part, (part + 1) * per_part):
            for load in loads[group]:
                load.wait()
            upward(group)
        if part == 0:
            pl.semaphore_wait(barrier, len(greeted) + crosses.astype(jnp.int32) + ends_line.astype(jnp.int32))

            @pl.when(ends_line)
            def _():
                pl.semaphore_signal(ready, inc=1, device_id=after, device_id_type=MESH)

        send("own pair", me, part, pair)
        send("own cross", me, part, cross, crosses)
        for phase, whom in enumerate(partners):
            send(("own", phase), me, part, whom)
        send("own sibling", me, part, sibling)

    for copy in (point_halos[0], coeff_halos[0]):
        copy.start()

    def send_back():
        for copy in (point_halos[1], coeff_halos[1]):
            copy.start()

    @pl.when(jnp.logical_not(starts_line))
    def _():
        send_back()

    def single(mask):
        return mask and mask & (mask - 1) == 0

    onward = []
    for step in range(line):
        up = planes[step] < my_z
        z = jnp.where(up, my_z + 1, my_z - 1)
        needed = (z >= 0) & (z < line)
        onward.append(((my_s, jnp.clip(z, 0, line - 1)), needed))

    def relay(mask, step, part):
        block = block_of(subset(mask), planes[step])
        arrived(block, part)
        if mask == 0:
            whom, needed = onward[step]
            send((mask, step, "onward"), block, part, whom, needed)
        if single(mask) and step == 0:
            send((mask, step, "pair"), block, part, pair, jnp.logical_not(crosses))
        if not (mask == 0 and step == 1):
            for phase in range(mask.bit_length(), nbits):
                send((mask, step, phase), block, part, partners[phase])
        send((mask, step, "sibling"), block, part, sibling)

    def relay_late(mask, step, part):
        send((mask, step, "late"), block_of(subset(mask), planes[step]), part, pair, crosses)

    def windows(mask, step):
        if nbits == 2 and line == 4:
            return MIDDLE[(mask, step)], END[(mask, step)]
        begin = 4 * bin(mask).count("1") + 3 * step
        return ((begin, begin + 3.0),) * 2

    events = []
    for step in range(line):
        for mask in range(1 << nbits):
            if mask or step:
                for part in range(parts):
                    action = functools.partial(relay, mask, step, part)
                    middle, end = [begin + (till - begin) * (part + 1) / parts for begin, till in windows(mask, step)]
                    if middle == end:
                        events.append((end, len(events), action))
                    else:
                        events.append((middle, len(events), functools.partial(when, crosses, action)))
                        events.append((end, len(events), functools.partial(when, jnp.logical_not(crosses), action)))
                    if single(mask) and step == 0:
                        begin = 6.0 if mask.bit_length() < nbits else 9.0
                        begin, till = LATE[mask] if nbits == 2 and line == 4 else (begin, begin + 3.0)
                        time = begin + (till - begin) * (part + 1) / parts
                        events.append((time, len(events), functools.partial(relay_late, mask, step, part)))

    def send_back_late():
        @pl.when(starts_line)
        def _():
            pl.semaphore_wait(ready, 1)
            send_back()

    events.append((READY_TIME, len(events), send_back_late))
    events.sort()

    clock = [CLOCK]

    def advance(time):
        clock[0] += time
        while events and events[0][0] <= clock[0]:
            events.pop(0)[2]()

    first = me == 0
    last = me == total_blocks - 1

    def near(group, rows_of, shift):
        cs = [group * width + i for i in range(width)]
        sums = []
        for c in cs:
            rows = [rows_of[c + shift + near_off[k, c]] for k in range(kn)]
            weights = [near_blocks[c, k] for k in range(kn)]
            sums.append(dot(jnp.concatenate(rows, axis=1), jnp.concatenate(weights, axis=1), NT))
        for c, value in zip(cs, sums):
            near_sum[c] = value

    def one_leaf(c, rows_of, shift):
        rows = [rows_of[c + shift + far_off[k, c]] for k in range(kc)]
        sides = [jnp.where(low_lanes, rows[k], rows[k + 1]) for k in range(0, kc, 2)]
        return dot(jnp.concatenate(sides, axis=1), leaf_panel[c], NT)

    def coupling(group, rows_of, shift):
        ps = [group * (width // 2) + i for i in range(width // 2)]
        pairs = [(one_leaf(2 * p, rows_of, shift), one_leaf(2 * p + 1, rows_of, shift)) for p in ps]
        for p, pair in zip(ps, pairs):
            leaf_sum[p] = jnp.concatenate(pair, axis=1)

    leaf_groups = leaves // width
    inner = list(range(1, leaf_groups - 1))
    for copy in indices:
        copy.wait()
    loaded = set()

    def near_piece(group, rows_of, shift):
        part = group * width // near_rows
        if part not in loaded:
            near_loads[part].wait()
            loaded.add(part)
        near(group, rows_of, shift)
        advance(NEAR_TIME)

    for group in inner:
        near_piece(group, points, 0)
    panels[0].wait()
    for group in inner:
        coupling(group, coeffs, 0)
        advance(FAR_TIME)

    advance(EDGE_TIME - clock[0])
    for copy in edges + point_halos + coeff_halos:
        copy.wait()

    @pl.when(first)
    def _():
        points_low[pl.ds(0, NEAR_REACH)] = jnp.zeros((NEAR_REACH, rhs, size), jnp.bfloat16)
        coeffs_low[pl.ds(0, FAR_REACH)] = jnp.zeros((FAR_REACH, rhs, 2 * rank), jnp.bfloat16)

    @pl.when(last)
    def _():
        points_high[pl.ds(near_edge, NEAR_REACH)] = jnp.zeros((NEAR_REACH, rhs, size), jnp.bfloat16)
        coeffs_high[pl.ds(far_edge, FAR_REACH)] = jnp.zeros((FAR_REACH, rhs, 2 * rank), jnp.bfloat16)

    near_piece(0, points_low, NEAR_REACH)
    near_piece(leaf_groups - 1, points_high, near_edge - leaves)
    coupling(0, coeffs_low, FAR_REACH)
    advance(FAR_TIME)
    coupling(leaf_groups - 1, coeffs_high, far_edge - leaves)
    advance(1e9)

    for h in range(1 << nbits):
        for z in range(line):
            for part in range(parts):
                arrived((h * 2 + 1 - core) * line + z, part)
    panels[1].wait()

    low_half = lax.broadcasted_iota(jnp.int32, (half, 2 * rank), 1) < rank

    def remote_rows(p):
        tiles = [gathered[owner[k, p] * parents + local[k, p]] for k in range(kp)]
        upper, lower = [], []
        for k in range(0, kp, 2):
            a, b = tiles[k], tiles[k + 1]
            turned_a = jnp.concatenate([a[:, rank:], a[:, :rank]], axis=1)
            turned_b = jnp.concatenate([b[:, rank:], b[:, :rank]], axis=1)
            upper.append(jnp.where(low_half, a, turned_b))
            lower.append(jnp.where(low_half, turned_a, b))
        return jnp.concatenate(
            [jnp.concatenate(upper, axis=1), jnp.concatenate(lower, axis=1)], axis=0)

    def downward(group, _):
        ps = [group * width + i for i in range(width)]
        fields = [dot(remote_rows(p), parent_panel[p], NT).astype(jnp.bfloat16) for p in ps]
        totals = [leaf_sum[p] + dot(field, transfer[p], NN) for p, field in zip(ps, fields)]
        fars = []
        for p, total in zip(ps, totals):
            zero = jnp.zeros_like(total)
            stacked = jnp.concatenate(
                [jnp.where(low_lanes, total, zero), jnp.where(low_lanes, zero, total)], axis=0)
            weights = basis[pl.ds(2 * p, 2)].reshape(2 * rank, size)
            fars.append(dot(stacked.astype(jnp.bfloat16), weights, NN))
        for p, far in zip(ps, fars):
            out[2 * p] = (far[:rhs] + near_sum[2 * p]).astype(jnp.bfloat16)
            out[2 * p + 1] = (far[rhs:] + near_sum[2 * p + 1]).astype(jnp.bfloat16)
        return 0

    for part in range(groups):
        downward(part, 0)
    for index, condition in sends.values():
        when(condition, functools.partial(sent, index))


def on_device(
    streams,
    line,
    points_rhs,
    leaf_basis,
    transfer,
    leaf_coupling,
    parent_coupling,
    near_blocks,
    near_offsets,
    coupling_offsets,
    parent_owner,
    parent_local,
):
    leaves, rhs, size = points_rhs.shape
    parents, rank, _ = transfer.shape
    places = streams // 2
    nbits = bits_of(places)
    blocks = streams * line
    parts, near_parts = PARTS, 4
    copies = sends_of(line, nbits) * parts
    hbm = pl.BlockSpec(memory_space=pltpu.HBM)
    bf16 = jnp.bfloat16
    dma = pltpu.SemaphoreType.DMA
    near_edge, far_edge = WIDTH + NEAR_REACH, WIDTH + FAR_REACH
    groups = parents // WIDTH
    offsets = [x.T for x in (near_offsets, coupling_offsets, parent_owner, parent_local)]
    return pl.pallas_call(
        functools.partial(kernel, streams, line, parts),
        out_shape=jax.ShapeDtypeStruct(points_rhs.shape, bf16),
        in_specs=[hbm] * 10,
        out_specs=pl.BlockSpec(memory_space=pltpu.VMEM),
        scratch_shapes=[
            *[pltpu.SMEM(x.shape, jnp.int32) for x in offsets],
            pltpu.VMEM(points_rhs.shape, bf16),
            pltpu.VMEM((near_edge + NEAR_REACH, rhs, size), bf16),
            pltpu.VMEM((near_edge + NEAR_REACH, rhs, size), bf16),
            pltpu.VMEM(leaf_basis.shape, bf16),
            pltpu.VMEM(transfer.shape, bf16),
            pltpu.VMEM(leaf_coupling.shape, bf16),
            pltpu.VMEM(parent_coupling.shape, bf16),
            pltpu.VMEM(near_blocks.shape, bf16),
            pltpu.VMEM((leaves, rhs, 2 * rank), bf16),
            pltpu.VMEM((far_edge + FAR_REACH, rhs, 2 * rank), bf16),
            pltpu.VMEM((far_edge + FAR_REACH, rhs, 2 * rank), bf16),
            pltpu.VMEM((blocks * parents, rhs // 2, 2 * rank), bf16),
            pltpu.VMEM((leaves, rhs, size), jnp.float32),
            pltpu.VMEM((parents, rhs, 2 * rank), jnp.float32),
            dma((4,)),
            dma((3 * groups,)),
            dma((2,)),
            dma((near_parts,)),
            dma((2,)),
            dma((4,)),
            dma((4,)),
            dma((copies,)),
            dma((blocks * parts,)),
            pltpu.SemaphoreType.REGULAR,
        ],
        compiler_params=pltpu.CompilerParams(
            collective_id=0, has_side_effects=True, vmem_limit_bytes=VMEM_LIMIT),
    )(
        *[pltpu.with_memory_space_constraint(x, pltpu.HBM) for x in (
            *offsets, points_rhs, leaf_basis, transfer, leaf_coupling, parent_coupling, near_blocks)]
    )


def solution(mesh):
    whole = P(("stream", "leaf"))
    return jax.shard_map(
        functools.partial(on_device, mesh.shape["stream"], mesh.shape["leaf"]),
        mesh=mesh,
        in_specs=(whole,) * 10,
        out_specs=whole,
        check_vma=False,
    )
```

```python
import functools

import jax
import jax.numpy as jnp
from jax import lax
from jax.experimental import pallas as pl
from jax.experimental.pallas import tpu as pltpu
from jax.sharding import PartitionSpec as P

NEAR_REACH = 2
FAR_REACH = 5
MESH = pl.DeviceIdType.MESH
NT = (((1,), (1,)), ((), ()))
NN = (((1,), (0,)), ((), ()))


WIDTH = 8
VMEM_LIMIT = 40 << 20
PARTS = 4
CLOCK, NEAR_TIME, FAR_TIME = 1.0, 0.8, 0.4
READY_TIME, EDGE_TIME = 4.4, 14.2
MIDDLE = {
    (0, 1): (1.2, 4.0),
    (1, 0): (2.3, 4.8),
    (2, 0): (2.3, 4.8),
    (0, 2): (0.6, 2.8),
    (0, 3): (4.0, 8.0),
    (1, 2): (5.0, 9.0),
    (2, 2): (9.5, 11.0),
    (1, 1): (11.0, 13.0),
    (1, 3): (11.0, 13.0),
    (2, 1): (13.0, 14.0),
    (2, 3): (12.5, 14.0),
    (3, 0): (13.9, 14.1),
    (3, 2): (14.4, 15.0),
    (3, 1): (15.0, 17.0),
    (3, 3): (15.5, 17.5),
}
END = {
    (0, 1): (2.3, 4.8),
    (1, 0): (2.3, 4.8),
    (2, 0): (2.3, 4.8),
    (0, 2): (3.5, 6.0),
    (0, 3): (6.0, 9.0),
    (1, 2): (9.5, 11.0),
    (2, 2): (9.5, 11.0),
    (1, 1): (11.0, 13.0),
    (1, 3): (11.0, 13.0),
    (2, 1): (13.0, 14.0),
    (2, 3): (12.5, 14.0),
    (3, 0): (13.9, 14.1),
    (3, 2): (14.4, 15.0),
    (3, 1): (15.0, 17.0),
    (3, 3): (15.5, 17.5),
}
LATE = {1: (8.2, 8.6), 2: (9.0, 10.0)}


def line_order(line):
    table = [sorted(range(line), key=lambda other: ((other // 2 != z // 2) + (other != z), abs(other - z), other))
             for z in range(line)]
    for z in range(line):
        for other in range(line):
            if abs(other - z) > 1:
                nearer = z + (1 if other > z else -1)
                assert table[nearer].index(other) <= table[z].index(other)
    return table


def sends_of(line, nbits):
    sends = nbits + 3
    for step in range(line):
        for mask in range(1 << nbits):
            if mask or step:
                sends += 1 + (mask == 0)
                sends += 2 * bool(mask and mask & (mask - 1) == 0 and step == 0)
                sends += 0 if mask == 0 and step == 1 else nbits - mask.bit_length()
    return sends


def dot(a, b, dims):
    return lax.dot_general(a, b, dims, preferred_element_type=jnp.float32)


def bits_of(count):
    bits = count.bit_length() - 1
    assert 1 << bits == count
    return bits


def kernel(
    streams, line, parts,
    near_off_hbm, far_off_hbm, owner_hbm, local_hbm,
    points_hbm, basis_hbm, transfer_hbm, leaf_hbm, parent_hbm, near_hbm,
    out,
    near_off, far_off, owner, local,
    points, points_low, points_high, basis, transfer, leaf_panel, parent_panel, near_blocks,
    coeffs, coeffs_low, coeffs_high, gathered, near_sum, leaf_sum,
    index_sem, load_sem, edge_sem, near_sem, panel_sem,
    halo_send, halo_recv, send_sem, recv_sem, sibling_sem, ready,
):
    leaves, rhs, size = points_hbm.shape
    parents, rank, _ = transfer_hbm.shape
    kn = near_off.shape[0]
    kc = far_off.shape[0]
    kp = owner.shape[0]
    half = rhs // 2
    width = WIDTH
    groups = parents // width
    near_edge = points_low.shape[0] - NEAR_REACH
    far_edge = coeffs_low.shape[0] - FAR_REACH
    chunk = parents // parts
    nbits = bits_of(streams // 2)
    bits_of(line)
    assert line > 1
    near_parts = near_sem.shape[0]

    my_s = lax.axis_index("stream")
    my_z = lax.axis_index("leaf")
    core = my_s % 2
    place = my_s // 2
    total_blocks = streams * line
    me = my_s * line + my_z

    def device(block):
        return (block // line, block % line)

    def block_of(h, z):
        return (h * 2 + core) * line + z

    def bit_at(phase):
        first = 1 << phase
        if nbits < 2:
            return first
        second = 1 << ((phase + 1) % nbits)
        return first + core * (second - first)

    def flip(h, bit):
        return h + bit * (1 - 2 * ((h // bit) % 2))

    def subset(mask):
        h = place
        for phase in range(nbits):
            if mask >> phase & 1:
                h = flip(h, bit_at(phase))
        return h

    table = line_order(line)
    planes = [my_z]
    for step in range(1, line):
        z = table[0][step]
        for row in range(1, line):
            z = jnp.where(my_z == row, table[row][step], z)
        planes.append(z)
    pair_z = flip(my_z, 1)
    cross_z = 2 * my_z - pair_z
    crosses = (cross_z >= 0) & (cross_z < line)
    ends = (cross_z < 0) | (cross_z >= line)
    cross_z = jnp.clip(cross_z, 0, line - 1)

    partners = [(flip(place, bit_at(i)) * 2 + core, my_z) for i in range(nbits)]
    pair = (my_s, pair_z)
    cross = (my_s, cross_z)
    sibling = (my_s + 1 - 2 * core, my_z)
    after = device((me + 1) % total_blocks)
    before = device((me + total_blocks - 1) % total_blocks)
    starts_line = my_z == 0
    ends_line = my_z == line - 1

    indices = [
        pltpu.make_async_copy(source, target, index_sem.at[i])
        for i, (source, target) in enumerate([
            (near_off_hbm, near_off), (far_off_hbm, far_off),
            (owner_hbm, owner), (local_hbm, local)])
    ]
    loads = [
        [pltpu.make_async_copy(source.at[pl.ds(g * step, step)],
                               target.at[pl.ds(g * step, step)], load_sem.at[3 * g + i])
         for i, (source, target, step) in enumerate([
             (points_hbm, points, 2 * width), (basis_hbm, basis, 2 * width),
             (transfer_hbm, transfer, width)])]
        for g in range(groups)
    ]
    edges = [
        pltpu.make_async_copy(points_hbm.at[pl.ds(0, near_edge)],
                              points_low.at[pl.ds(NEAR_REACH, near_edge)], edge_sem.at[0]),
        pltpu.make_async_copy(points_hbm.at[pl.ds(leaves - near_edge, near_edge)],
                              points_high.at[pl.ds(0, near_edge)], edge_sem.at[1]),
    ]
    panels = [
        pltpu.make_async_copy(leaf_hbm, leaf_panel, panel_sem.at[0]),
        pltpu.make_async_copy(parent_hbm, parent_panel, panel_sem.at[1]),
    ]
    near_rows = leaves // near_parts
    near_loads = [
        pltpu.make_async_copy(
            near_hbm.at[pl.ds(i * near_rows, near_rows)],
            near_blocks.at[pl.ds(i * near_rows, near_rows)],
            near_sem.at[i],
        )
        for i in range(near_parts)
    ]
    barrier = pltpu.get_barrier_semaphore()
    for load in loads[0]:
        load.start()
    greeted = partners + [pair, sibling]
    for other in greeted:
        pl.semaphore_signal(barrier, inc=1, device_id=other, device_id_type=MESH)

    @pl.when(crosses)
    def _():
        pl.semaphore_signal(barrier, inc=1, device_id=cross, device_id_type=MESH)

    @pl.when(starts_line)
    def _():
        pl.semaphore_signal(barrier, inc=1, device_id=before, device_id_type=MESH)

    for group in loads[1:]:
        for load in group:
            load.start()
    for load in indices + edges + near_loads + panels:
        load.start()

    low_lanes = lax.broadcasted_iota(jnp.int32, (rhs, 2 * rank), 1) < rank

    def upward(group):
        ps = [group * width + i for i in range(width)]
        boths = []
        for p in ps:
            pair = jnp.concatenate([points[2 * p], points[2 * p + 1]], axis=0)
            weights = basis[pl.ds(2 * p, 2)].reshape(2 * rank, size)
            boths.append(dot(pair, weights, NT))
        sides = [jnp.where(low_lanes, both[:rhs], both[rhs:]) for both in boths]
        ups = [dot(side.astype(jnp.bfloat16), transfer[p], NT) for p, side in zip(ps, sides)]
        for p, up in zip(ps, ups):
            packed = jnp.concatenate([up[:half], up[half:]], axis=1)
            gathered[me * parents + p] = packed.astype(jnp.bfloat16)
        for p, side in zip(ps, sides):
            rolled = pltpu.roll(side, rank, 1)
            for c, value in ((2 * p, jnp.where(low_lanes, side, rolled).astype(jnp.bfloat16)),
                             (2 * p + 1, jnp.where(low_lanes, rolled, side).astype(jnp.bfloat16))):
                coeffs[c] = value
                if c < far_edge:
                    coeffs_low[FAR_REACH + c] = value
                if c >= leaves - far_edge:
                    coeffs_high[c - (leaves - far_edge)] = value

    def halo(index, source, target, whom):
        return pltpu.make_async_remote_copy(
            src_ref=source, dst_ref=target,
            send_sem=halo_send.at[index], recv_sem=halo_recv.at[index],
            device_id=whom, device_id_type=MESH,
        )

    point_halos = [
        halo(0, points.at[pl.ds(leaves - NEAR_REACH, NEAR_REACH)],
             points_low.at[pl.ds(0, NEAR_REACH)], after),
        halo(1, points.at[pl.ds(0, NEAR_REACH)],
             points_high.at[pl.ds(near_edge, NEAR_REACH)], before),
    ]
    coeff_halos = [
        halo(2, coeffs.at[pl.ds(leaves - FAR_REACH, FAR_REACH)],
             coeffs_low.at[pl.ds(0, FAR_REACH)], after),
        halo(3, coeffs.at[pl.ds(0, FAR_REACH)],
             coeffs_high.at[pl.ds(far_edge, FAR_REACH)], before),
    ]

    sends = {}

    def when(condition, action):
        if condition is None:
            action()
        else:
            pl.when(condition)(action)

    def span(block, part):
        return gathered.at[pl.ds(block * parents + part * chunk, chunk)]

    tallies = {}

    def send(name, block, part, whom, condition=None, group="all"):
        if group == "all":
            group = (group, len([1 for other in sends.values() if other[0] == "all"]) // (total_blocks * parts))
        group = sends.setdefault((name, part), group)
        index, _ = tallies.setdefault(group, (len(tallies), condition))
        arrives = sibling_sem.at[0] if whom is sibling else recv_sem.at[slot(block, part)]
        when(condition, pltpu.make_async_remote_copy(
            src_ref=span(block, part), dst_ref=span(block, part),
            send_sem=send_sem.at[index], recv_sem=arrives,
            device_id=whom, device_id_type=MESH,
        ).start)

    def slot(block, part):
        return (block // (2 * line) * line + block % line) * parts + part

    def moved(rows, sent, received):
        return pltpu.make_async_remote_copy(
            src_ref=gathered.at[pl.ds(0, rows)], dst_ref=gathered.at[pl.ds(0, rows)],
            send_sem=sent, recv_sem=received, device_id=sibling, device_id_type=MESH)

    def arrived(block, part):
        moved(chunk, send_sem.at[0], recv_sem.at[slot(block, part)]).wait_recv()

    per_part = groups // parts
    for part in range(parts):
        for group in range(part * per_part, (part + 1) * per_part):
            for load in loads[group]:
                load.wait()
            upward(group)
        if part == 0:
            pl.semaphore_wait(barrier, len(greeted) + crosses.astype(jnp.int32) + ends_line.astype(jnp.int32))

            @pl.when(ends_line)
            def _():
                pl.semaphore_signal(ready, inc=1, device_id=after, device_id_type=MESH)

        send("own pair", me, part, pair)
        send("own cross", me, part, cross, crosses, "crosses")
        for phase, whom in enumerate(partners):
            send(("own", phase), me, part, whom)
        send("own sibling", me, part, sibling)

    for copy in (point_halos[0], coeff_halos[0]):
        copy.start()

    def send_back():
        for copy in (point_halos[1], coeff_halos[1]):
            copy.start()

    @pl.when(jnp.logical_not(starts_line))
    def _():
        send_back()

    def single(mask):
        return mask and mask & (mask - 1) == 0

    onward = []
    for step in range(line):
        up = planes[step] < my_z
        z = jnp.where(up, my_z + 1, my_z - 1)
        needed = (z >= 0) & (z < line)
        onward.append(((my_s, jnp.clip(z, 0, line - 1)), needed))

    def relay(mask, step, part):
        block = block_of(subset(mask), planes[step])
        arrived(block, part)
        if mask == 0:
            whom, needed = onward[step]
            send((mask, step, "onward"), block, part, whom, needed, ("onward", step))
        if single(mask) and step == 0:
            send((mask, step, "pair"), block, part, pair, ends, "ends")
        if not (mask == 0 and step == 1):
            for phase in range(mask.bit_length(), nbits):
                send((mask, step, phase), block, part, partners[phase])
        send((mask, step, "sibling"), block, part, sibling)

    def relay_late(mask, step, part):
        send((mask, step, "late"), block_of(subset(mask), planes[step]), part, pair, crosses, "crosses")

    def windows(mask, step):
        if nbits == 2 and line == 4:
            return MIDDLE[(mask, step)], END[(mask, step)]
        begin = 4 * bin(mask).count("1") + 3 * step
        return ((begin, begin + 3.0),) * 2

    events = []
    for step in range(line):
        for mask in range(1 << nbits):
            if mask or step:
                for part in range(parts):
                    action = functools.partial(relay, mask, step, part)
                    middle, end = [begin + (till - begin) * (part + 1) / parts for begin, till in windows(mask, step)]
                    if middle == end:
                        events.append((end, len(events), action))
                    else:
                        events.append((middle, len(events), functools.partial(when, crosses, action)))
                        events.append((end, len(events), functools.partial(when, jnp.logical_not(crosses), action)))
                    if single(mask) and step == 0:
                        begin = 6.0 if mask.bit_length() < nbits else 9.0
                        begin, till = LATE[mask] if nbits == 2 and line == 4 else (begin, begin + 3.0)
                        time = begin + (till - begin) * (part + 1) / parts
                        events.append((time, len(events), functools.partial(relay_late, mask, step, part)))

    def send_back_late():
        @pl.when(starts_line)
        def _():
            pl.semaphore_wait(ready, 1)
            send_back()

    events.append((READY_TIME, len(events), send_back_late))
    events.sort()

    clock = [CLOCK]

    def advance(time):
        clock[0] += time
        while events and events[0][0] <= clock[0]:
            events.pop(0)[2]()

    first = me == 0
    last = me == total_blocks - 1

    def near(group, rows_of, shift):
        cs = [group * width + i for i in range(width)]
        sums = []
        for c in cs:
            rows = [rows_of[c + shift + near_off[k, c]] for k in range(kn)]
            weights = [near_blocks[c, k] for k in range(kn)]
            sums.append(dot(jnp.concatenate(rows, axis=1), jnp.concatenate(weights, axis=1), NT))
        for c, value in zip(cs, sums):
            near_sum[c] = value

    def one_leaf(c, rows_of, shift):
        rows = [rows_of[c + shift + far_off[k, c]] for k in range(kc)]
        sides = [jnp.where(low_lanes, rows[k], rows[k + 1]) for k in range(0, kc, 2)]
        return dot(jnp.concatenate(sides, axis=1), leaf_panel[c], NT)

    def coupling(group, rows_of, shift):
        ps = [group * (width // 2) + i for i in range(width // 2)]
        pairs = [(one_leaf(2 * p, rows_of, shift), one_leaf(2 * p + 1, rows_of, shift)) for p in ps]
        for p, pair in zip(ps, pairs):
            leaf_sum[p] = jnp.concatenate(pair, axis=1)

    leaf_groups = leaves // width
    inner = list(range(1, leaf_groups - 1))
    for copy in indices:
        copy.wait()
    loaded = set()

    def near_piece(group, rows_of, shift):
        part = group * width // near_rows
        if part not in loaded:
            near_loads[part].wait()
            loaded.add(part)
        near(group, rows_of, shift)
        advance(NEAR_TIME)

    for group in inner:
        near_piece(group, points, 0)
    panels[0].wait()
    for group in inner:
        coupling(group, coeffs, 0)
        advance(FAR_TIME)

    advance(EDGE_TIME - clock[0])
    for copy in edges + point_halos + coeff_halos:
        copy.wait()

    @pl.when(first)
    def _():
        points_low[pl.ds(0, NEAR_REACH)] = jnp.zeros((NEAR_REACH, rhs, size), jnp.bfloat16)
        coeffs_low[pl.ds(0, FAR_REACH)] = jnp.zeros((FAR_REACH, rhs, 2 * rank), jnp.bfloat16)

    @pl.when(last)
    def _():
        points_high[pl.ds(near_edge, NEAR_REACH)] = jnp.zeros((NEAR_REACH, rhs, size), jnp.bfloat16)
        coeffs_high[pl.ds(far_edge, FAR_REACH)] = jnp.zeros((FAR_REACH, rhs, 2 * rank), jnp.bfloat16)

    near_piece(0, points_low, NEAR_REACH)
    near_piece(leaf_groups - 1, points_high, near_edge - leaves)
    coupling(0, coeffs_low, FAR_REACH)
    advance(FAR_TIME)
    coupling(leaf_groups - 1, coeffs_high, far_edge - leaves)
    advance(1e9)

    moved(total_blocks // 2 * parents, send_sem.at[0], sibling_sem.at[0]).wait_recv()
    panels[1].wait()

    low_half = lax.broadcasted_iota(jnp.int32, (half, 2 * rank), 1) < rank

    def remote_rows(p):
        tiles = [gathered[owner[k, p] * parents + local[k, p]] for k in range(kp)]
        upper, lower = [], []
        for k in range(0, kp, 2):
            a, b = tiles[k], tiles[k + 1]
            turned_a = jnp.concatenate([a[:, rank:], a[:, :rank]], axis=1)
            turned_b = jnp.concatenate([b[:, rank:], b[:, :rank]], axis=1)
            upper.append(jnp.where(low_half, a, turned_b))
            lower.append(jnp.where(low_half, turned_a, b))
        return jnp.concatenate(
            [jnp.concatenate(upper, axis=1), jnp.concatenate(lower, axis=1)], axis=0)

    def downward(group, _):
        ps = [group * width + i for i in range(width)]
        fields = [dot(remote_rows(p), parent_panel[p], NT).astype(jnp.bfloat16) for p in ps]
        totals = [leaf_sum[p] + dot(field, transfer[p], NN) for p, field in zip(ps, fields)]
        fars = []
        for p, total in zip(ps, totals):
            zero = jnp.zeros_like(total)
            stacked = jnp.concatenate(
                [jnp.where(low_lanes, total, zero), jnp.where(low_lanes, zero, total)], axis=0)
            weights = basis[pl.ds(2 * p, 2)].reshape(2 * rank, size)
            fars.append(dot(stacked.astype(jnp.bfloat16), weights, NN))
        for p, far in zip(ps, fars):
            out[2 * p] = (far[:rhs] + near_sum[2 * p]).astype(jnp.bfloat16)
            out[2 * p + 1] = (far[rhs:] + near_sum[2 * p + 1]).astype(jnp.bfloat16)
        return 0

    for part in range(groups):
        downward(part, 0)
    for group, (index, condition) in tallies.items():
        rows = chunk * list(sends.values()).count(group)
        when(condition, moved(rows, send_sem.at[index], sibling_sem.at[0]).wait_send)


def on_device(
    streams,
    line,
    points_rhs,
    leaf_basis,
    transfer,
    leaf_coupling,
    parent_coupling,
    near_blocks,
    near_offsets,
    coupling_offsets,
    parent_owner,
    parent_local,
):
    leaves, rhs, size = points_rhs.shape
    parents, rank, _ = transfer.shape
    places = streams // 2
    nbits = bits_of(places)
    blocks = streams * line
    parts, near_parts = PARTS, 4
    hbm = pl.BlockSpec(memory_space=pltpu.HBM)
    bf16 = jnp.bfloat16
    dma = pltpu.SemaphoreType.DMA
    near_edge, far_edge = WIDTH + NEAR_REACH, WIDTH + FAR_REACH
    groups = parents // WIDTH
    offsets = [x.T for x in (near_offsets, coupling_offsets, parent_owner, parent_local)]
    return pl.pallas_call(
        functools.partial(kernel, streams, line, parts),
        out_shape=jax.ShapeDtypeStruct(points_rhs.shape, bf16),
        in_specs=[hbm] * 10,
        out_specs=pl.BlockSpec(memory_space=pltpu.VMEM),
        scratch_shapes=[
            *[pltpu.SMEM(x.shape, jnp.int32) for x in offsets],
            pltpu.VMEM(points_rhs.shape, bf16),
            pltpu.VMEM((near_edge + NEAR_REACH, rhs, size), bf16),
            pltpu.VMEM((near_edge + NEAR_REACH, rhs, size), bf16),
            pltpu.VMEM(leaf_basis.shape, bf16),
            pltpu.VMEM(transfer.shape, bf16),
            pltpu.VMEM(leaf_coupling.shape, bf16),
            pltpu.VMEM(parent_coupling.shape, bf16),
            pltpu.VMEM(near_blocks.shape, bf16),
            pltpu.VMEM((leaves, rhs, 2 * rank), bf16),
            pltpu.VMEM((far_edge + FAR_REACH, rhs, 2 * rank), bf16),
            pltpu.VMEM((far_edge + FAR_REACH, rhs, 2 * rank), bf16),
            pltpu.VMEM((blocks * parents, rhs // 2, 2 * rank), bf16),
            pltpu.VMEM((leaves, rhs, size), jnp.float32),
            pltpu.VMEM((parents, rhs, 2 * rank), jnp.float32),
            dma((4,)),
            dma((3 * groups,)),
            dma((2,)),
            dma((near_parts,)),
            dma((2,)),
            dma((4,)),
            dma((4,)),
            dma((line + 3 + sends_of(line, nbits) // blocks,)),
            dma((blocks // 2 * parts,)),
            dma((1,)),
            pltpu.SemaphoreType.REGULAR,
        ],
        compiler_params=pltpu.CompilerParams(
            collective_id=0, has_side_effects=True, vmem_limit_bytes=VMEM_LIMIT),
    )(
        *[pltpu.with_memory_space_constraint(x, pltpu.HBM) for x in (
            *offsets, points_rhs, leaf_basis, transfer, leaf_coupling, parent_coupling, near_blocks)]
    )


def solution(mesh):
    whole = P(("stream", "leaf"))
    return jax.shard_map(
        functools.partial(on_device, mesh.shape["stream"], mesh.shape["leaf"]),
        mesh=mesh,
        in_specs=(whole,) * 10,
        out_specs=whole,
        check_vma=False,
    )
```

```python
import functools

import jax
import jax.numpy as jnp
from jax import lax
from jax.experimental import pallas as pl
from jax.experimental.pallas import tpu as pltpu
from jax.sharding import PartitionSpec as P

NEAR_REACH = 2
FAR_REACH = 5
MESH = pl.DeviceIdType.MESH
NT = (((1,), (1,)), ((), ()))
NN = (((1,), (0,)), ((), ()))


WIDTH = 8
DOWN_WIDTH = 32
VMEM_LIMIT = 40 << 20
PARTS = 4
CLOCK, NEAR_TIME, FAR_TIME = 1.0, 0.8, 0.4
READY_TIME, EDGE_TIME = 4.4, 14.2
MIDDLE = {
    (0, 1): (1.2, 4.0),
    (1, 0): (2.3, 4.8),
    (2, 0): (2.3, 4.8),
    (0, 2): (0.6, 2.8),
    (0, 3): (4.0, 8.0),
    (1, 2): (5.0, 9.0),
    (2, 2): (12.0, 13.0),
    (1, 1): (11.5, 13.0),
    (1, 3): (11.0, 13.0),
    (2, 1): (13.0, 14.0),
    (2, 3): (12.5, 14.0),
    (3, 0): (13.9, 14.1),
    (3, 2): (14.4, 15.0),
    (3, 1): (15.0, 17.0),
    (3, 3): (15.5, 17.5),
}
END = {
    (0, 1): (2.3, 4.8),
    (1, 0): (2.3, 4.8),
    (2, 0): (2.3, 4.8),
    (0, 2): (3.5, 6.0),
    (0, 3): (6.0, 9.0),
    (1, 2): (9.5, 11.0),
    (2, 2): (12.0, 13.0),
    (1, 1): (11.5, 13.0),
    (1, 3): (11.0, 13.0),
    (2, 1): (13.0, 14.0),
    (2, 3): (12.5, 14.0),
    (3, 0): (13.9, 14.1),
    (3, 2): (14.4, 15.0),
    (3, 1): (15.0, 17.0),
    (3, 3): (15.5, 17.5),
}
LATE = {1: (8.2, 8.6), 2: (9.0, 10.0)}


def line_order(line):
    table = [sorted(range(line), key=lambda other: ((other // 2 != z // 2) + (other != z), abs(other - z), other))
             for z in range(line)]
    for z in range(line):
        for other in range(line):
            if abs(other - z) > 1:
                nearer = z + (1 if other > z else -1)
                assert table[nearer].index(other) <= table[z].index(other)
    return table


def sends_of(line, nbits):
    sends = nbits + 3
    for step in range(line):
        for mask in range(1 << nbits):
            if mask or step:
                sends += 1 + (mask == 0)
                sends += 2 * bool(mask and mask & (mask - 1) == 0 and step == 0)
                sends += 0 if mask == 0 and step == 1 else nbits - mask.bit_length()
    return sends


def dot(a, b, dims):
    return lax.dot_general(a, b, dims, preferred_element_type=jnp.float32)


def bits_of(count):
    bits = count.bit_length() - 1
    assert 1 << bits == count
    return bits


def kernel(
    streams, line, parts,
    near_off_hbm, far_off_hbm, owner_hbm, local_hbm,
    points_hbm, basis_hbm, transfer_hbm, leaf_hbm, parent_hbm, near_hbm,
    out,
    near_off, far_off, owner, local,
    points, points_low, points_high, basis, transfer, leaf_panel, parent_panel, near_blocks,
    coeffs, coeffs_low, coeffs_high, gathered, near_sum, leaf_sum,
    index_sem, load_sem, edge_sem, near_sem, panel_sem,
    halo_send, halo_recv, send_sem, recv_sem, sibling_sem, ready,
):
    leaves, rhs, size = points_hbm.shape
    parents, rank, _ = transfer_hbm.shape
    kn = near_off.shape[0]
    kc = far_off.shape[0]
    kp = owner.shape[0]
    half = rhs // 2
    width = WIDTH
    groups = parents // width
    near_edge = points_low.shape[0] - NEAR_REACH
    far_edge = coeffs_low.shape[0] - FAR_REACH
    chunk = parents // parts
    nbits = bits_of(streams // 2)
    bits_of(line)
    assert line > 1
    near_parts = near_sem.shape[0]

    my_s = lax.axis_index("stream")
    my_z = lax.axis_index("leaf")
    core = my_s % 2
    place = my_s // 2
    total_blocks = streams * line
    me = my_s * line + my_z

    def device(block):
        return (block // line, block % line)

    def block_of(h, z):
        return (h * 2 + core) * line + z

    def bit_at(phase):
        first = 1 << phase
        if nbits < 2:
            return first
        second = 1 << ((phase + 1) % nbits)
        return first + core * (second - first)

    def flip(h, bit):
        return h + bit * (1 - 2 * ((h // bit) % 2))

    def subset(mask):
        h = place
        for phase in range(nbits):
            if mask >> phase & 1:
                h = flip(h, bit_at(phase))
        return h

    table = line_order(line)
    planes = [my_z]
    for step in range(1, line):
        z = table[0][step]
        for row in range(1, line):
            z = jnp.where(my_z == row, table[row][step], z)
        planes.append(z)
    pair_z = flip(my_z, 1)
    cross_z = 2 * my_z - pair_z
    crosses = (cross_z >= 0) & (cross_z < line)
    ends = (cross_z < 0) | (cross_z >= line)
    cross_z = jnp.clip(cross_z, 0, line - 1)

    partners = [(flip(place, bit_at(i)) * 2 + core, my_z) for i in range(nbits)]
    pair = (my_s, pair_z)
    cross = (my_s, cross_z)
    sibling = (my_s + 1 - 2 * core, my_z)
    after = device((me + 1) % total_blocks)
    before = device((me + total_blocks - 1) % total_blocks)
    starts_line = my_z == 0
    ends_line = my_z == line - 1

    indices = [
        pltpu.make_async_copy(source, target, index_sem.at[i])
        for i, (source, target) in enumerate([
            (near_off_hbm, near_off), (far_off_hbm, far_off),
            (owner_hbm, owner), (local_hbm, local)])
    ]
    loads = [
        [pltpu.make_async_copy(source.at[pl.ds(g * step, step)],
                               target.at[pl.ds(g * step, step)], load_sem.at[3 * g + i])
         for i, (source, target, step) in enumerate([
             (points_hbm, points, 2 * width), (basis_hbm, basis, 2 * width),
             (transfer_hbm, transfer, width)])]
        for g in range(groups)
    ]
    edges = [
        pltpu.make_async_copy(points_hbm.at[pl.ds(0, near_edge)],
                              points_low.at[pl.ds(NEAR_REACH, near_edge)], edge_sem.at[0]),
        pltpu.make_async_copy(points_hbm.at[pl.ds(leaves - near_edge, near_edge)],
                              points_high.at[pl.ds(0, near_edge)], edge_sem.at[1]),
    ]
    panels = [
        pltpu.make_async_copy(leaf_hbm, leaf_panel, panel_sem.at[0]),
        pltpu.make_async_copy(parent_hbm, parent_panel, panel_sem.at[1]),
    ]
    near_rows = leaves // near_parts
    near_loads = [
        pltpu.make_async_copy(
            near_hbm.at[pl.ds(i * near_rows, near_rows)],
            near_blocks.at[pl.ds(i * near_rows, near_rows)],
            near_sem.at[i],
        )
        for i in range(near_parts)
    ]
    barrier = pltpu.get_barrier_semaphore()
    for load in loads[0]:
        load.start()
    greeted = partners + [pair, sibling]
    for other in greeted:
        pl.semaphore_signal(barrier, inc=1, device_id=other, device_id_type=MESH)

    @pl.when(crosses)
    def _():
        pl.semaphore_signal(barrier, inc=1, device_id=cross, device_id_type=MESH)

    @pl.when(starts_line)
    def _():
        pl.semaphore_signal(barrier, inc=1, device_id=before, device_id_type=MESH)

    for group in loads[1:]:
        for load in group:
            load.start()
    for load in indices + edges + near_loads + panels:
        load.start()

    low_lanes = lax.broadcasted_iota(jnp.int32, (rhs, 2 * rank), 1) < rank

    def upward(group):
        ps = [group * width + i for i in range(width)]
        boths = []
        for p in ps:
            pair = jnp.concatenate([points[2 * p], points[2 * p + 1]], axis=0)
            weights = basis[pl.ds(2 * p, 2)].reshape(2 * rank, size)
            boths.append(dot(pair, weights, NT))
        sides = [jnp.where(low_lanes, both[:rhs], both[rhs:]) for both in boths]
        ups = [dot(side.astype(jnp.bfloat16), transfer[p], NT) for p, side in zip(ps, sides)]
        for p, up in zip(ps, ups):
            packed = jnp.concatenate([up[:half], up[half:]], axis=1)
            gathered[me * parents + p] = packed.astype(jnp.bfloat16)
        for p, side in zip(ps, sides):
            rolled = pltpu.roll(side, rank, 1)
            for c, value in ((2 * p, jnp.where(low_lanes, side, rolled).astype(jnp.bfloat16)),
                             (2 * p + 1, jnp.where(low_lanes, rolled, side).astype(jnp.bfloat16))):
                coeffs[c] = value
                if c < far_edge:
                    coeffs_low[FAR_REACH + c] = value
                if c >= leaves - far_edge:
                    coeffs_high[c - (leaves - far_edge)] = value

    def halo(index, source, target, whom):
        return pltpu.make_async_remote_copy(
            src_ref=source, dst_ref=target,
            send_sem=halo_send.at[index], recv_sem=halo_recv.at[index],
            device_id=whom, device_id_type=MESH,
        )

    point_halos = [
        halo(0, points.at[pl.ds(leaves - NEAR_REACH, NEAR_REACH)],
             points_low.at[pl.ds(0, NEAR_REACH)], after),
        halo(1, points.at[pl.ds(0, NEAR_REACH)],
             points_high.at[pl.ds(near_edge, NEAR_REACH)], before),
    ]
    coeff_halos = [
        halo(2, coeffs.at[pl.ds(leaves - FAR_REACH, FAR_REACH)],
             coeffs_low.at[pl.ds(0, FAR_REACH)], after),
        halo(3, coeffs.at[pl.ds(0, FAR_REACH)],
             coeffs_high.at[pl.ds(far_edge, FAR_REACH)], before),
    ]

    sends = {}

    def when(condition, action):
        if condition is None:
            action()
        else:
            pl.when(condition)(action)

    def span(block, part):
        return gathered.at[pl.ds(block * parents + part * chunk, chunk)]

    tallies = {}

    def send(name, block, part, whom, condition=None, group="all"):
        if group == "all":
            group = (group, len([1 for other in sends.values() if other[0] == "all"]) // (total_blocks * parts))
        group = sends.setdefault((name, part), group)
        index, _ = tallies.setdefault(group, (len(tallies), condition))
        arrives = sibling_sem.at[0] if whom is sibling else recv_sem.at[slot(block, part)]
        when(condition, pltpu.make_async_remote_copy(
            src_ref=span(block, part), dst_ref=span(block, part),
            send_sem=send_sem.at[index], recv_sem=arrives,
            device_id=whom, device_id_type=MESH,
        ).start)

    def slot(block, part):
        return (block // (2 * line) * line + block % line) * parts + part

    def moved(rows, sent, received):
        return pltpu.make_async_remote_copy(
            src_ref=gathered.at[pl.ds(0, rows)], dst_ref=gathered.at[pl.ds(0, rows)],
            send_sem=sent, recv_sem=received, device_id=sibling, device_id_type=MESH)

    def arrived(block, part):
        moved(chunk, send_sem.at[0], recv_sem.at[slot(block, part)]).wait_recv()

    per_part = groups // parts
    for part in range(parts):
        for group in range(part * per_part, (part + 1) * per_part):
            for load in loads[group]:
                load.wait()
            upward(group)
        if part == 0:
            pl.semaphore_wait(barrier, len(greeted) + crosses.astype(jnp.int32) + ends_line.astype(jnp.int32))

            @pl.when(ends_line)
            def _():
                pl.semaphore_signal(ready, inc=1, device_id=after, device_id_type=MESH)

        send("own pair", me, part, pair)
        send("own cross", me, part, cross, crosses, "crosses")
        for phase, whom in enumerate(partners):
            send(("own", phase), me, part, whom)
        send("own sibling", me, part, sibling)

    for copy in (point_halos[0], coeff_halos[0]):
        copy.start()

    def send_back():
        for copy in (point_halos[1], coeff_halos[1]):
            copy.start()

    @pl.when(jnp.logical_not(starts_line))
    def _():
        send_back()

    def single(mask):
        return mask and mask & (mask - 1) == 0

    onward = []
    for step in range(line):
        up = planes[step] < my_z
        z = jnp.where(up, my_z + 1, my_z - 1)
        needed = (z >= 0) & (z < line)
        onward.append(((my_s, jnp.clip(z, 0, line - 1)), needed))

    def relay(mask, step, part):
        block = block_of(subset(mask), planes[step])
        arrived(block, part)
        if mask == 0:
            whom, needed = onward[step]
            send((mask, step, "onward"), block, part, whom, needed, ("onward", step))
        if single(mask) and step == 0:
            send((mask, step, "pair"), block, part, pair, ends, "ends")
        if not (mask == 0 and step == 1):
            for phase in range(mask.bit_length(), nbits):
                send((mask, step, phase), block, part, partners[phase])
        send((mask, step, "sibling"), block, part, sibling)

    def relay_late(mask, step, part):
        send((mask, step, "late"), block_of(subset(mask), planes[step]), part, pair, crosses, "crosses")

    def windows(mask, step):
        if nbits == 2 and line == 4:
            return MIDDLE[(mask, step)], END[(mask, step)]
        begin = 4 * bin(mask).count("1") + 3 * step
        return ((begin, begin + 3.0),) * 2

    events = []
    for step in range(line):
        for mask in range(1 << nbits):
            if mask or step:
                for part in range(parts):
                    action = functools.partial(relay, mask, step, part)
                    middle, end = [begin + (till - begin) * (part + 1) / parts for begin, till in windows(mask, step)]
                    if middle == end:
                        events.append((end, len(events), action))
                    else:
                        events.append((middle, len(events), functools.partial(when, crosses, action)))
                        events.append((end, len(events), functools.partial(when, jnp.logical_not(crosses), action)))
                    if single(mask) and step == 0:
                        begin = 6.0 if mask.bit_length() < nbits else 9.0
                        begin, till = LATE[mask] if nbits == 2 and line == 4 else (begin, begin + 3.0)
                        time = begin + (till - begin) * (part + 1) / parts
                        events.append((time, len(events), functools.partial(relay_late, mask, step, part)))

    def send_back_late():
        @pl.when(starts_line)
        def _():
            pl.semaphore_wait(ready, 1)
            send_back()

    events.append((READY_TIME, len(events), send_back_late))
    events.sort()

    clock = [CLOCK]

    def advance(time):
        clock[0] += time
        while events and events[0][0] <= clock[0]:
            events.pop(0)[2]()

    first = me == 0
    last = me == total_blocks - 1

    def near(group, rows_of, shift):
        cs = [group * width + i for i in range(width)]
        sums = []
        for c in cs:
            rows = [rows_of[c + shift + near_off[k, c]] for k in range(kn)]
            weights = [near_blocks[c, k] for k in range(kn)]
            sums.append(dot(jnp.concatenate(rows, axis=1), jnp.concatenate(weights, axis=1), NT))
        for c, value in zip(cs, sums):
            near_sum[c] = value

    def one_leaf(c, rows_of, shift):
        rows = [rows_of[c + shift + far_off[k, c]] for k in range(kc)]
        sides = [jnp.where(low_lanes, rows[k], rows[k + 1]) for k in range(0, kc, 2)]
        return dot(jnp.concatenate(sides, axis=1), leaf_panel[c], NT)

    def coupling(group, rows_of, shift):
        ps = [group * (width // 2) + i for i in range(width // 2)]
        pairs = [(one_leaf(2 * p, rows_of, shift), one_leaf(2 * p + 1, rows_of, shift)) for p in ps]
        for p, pair in zip(ps, pairs):
            leaf_sum[p] = jnp.concatenate(pair, axis=1)

    leaf_groups = leaves // width
    inner = list(range(1, leaf_groups - 1))
    for copy in indices:
        copy.wait()
    loaded = set()

    def near_piece(group, rows_of, shift):
        part = group * width // near_rows
        if part not in loaded:
            near_loads[part].wait()
            loaded.add(part)
        near(group, rows_of, shift)
        advance(NEAR_TIME)

    for group in inner:
        near_piece(group, points, 0)
    panels[0].wait()
    for group in inner:
        coupling(group, coeffs, 0)
        advance(FAR_TIME)

    advance(EDGE_TIME - clock[0])
    for copy in edges + point_halos + coeff_halos:
        copy.wait()

    @pl.when(first)
    def _():
        points_low[pl.ds(0, NEAR_REACH)] = jnp.zeros((NEAR_REACH, rhs, size), jnp.bfloat16)
        coeffs_low[pl.ds(0, FAR_REACH)] = jnp.zeros((FAR_REACH, rhs, 2 * rank), jnp.bfloat16)

    @pl.when(last)
    def _():
        points_high[pl.ds(near_edge, NEAR_REACH)] = jnp.zeros((NEAR_REACH, rhs, size), jnp.bfloat16)
        coeffs_high[pl.ds(far_edge, FAR_REACH)] = jnp.zeros((FAR_REACH, rhs, 2 * rank), jnp.bfloat16)

    near_piece(0, points_low, NEAR_REACH)
    near_piece(leaf_groups - 1, points_high, near_edge - leaves)
    coupling(0, coeffs_low, FAR_REACH)
    advance(FAR_TIME)
    coupling(leaf_groups - 1, coeffs_high, far_edge - leaves)
    advance(1e9)

    moved(total_blocks // 2 * parents, send_sem.at[0], sibling_sem.at[0]).wait_recv()
    panels[1].wait()

    low_half = lax.broadcasted_iota(jnp.int32, (half, 2 * rank), 1) < rank

    def remote_rows(p):
        tiles = [gathered[owner[k, p] * parents + local[k, p]] for k in range(kp)]
        upper, lower = [], []
        for k in range(0, kp, 2):
            a, b = tiles[k], tiles[k + 1]
            turned_a = jnp.concatenate([a[:, rank:], a[:, :rank]], axis=1)
            turned_b = jnp.concatenate([b[:, rank:], b[:, :rank]], axis=1)
            upper.append(jnp.where(low_half, a, turned_b))
            lower.append(jnp.where(low_half, turned_a, b))
        return jnp.concatenate(
            [jnp.concatenate(upper, axis=1), jnp.concatenate(lower, axis=1)], axis=0)

    def downward(group):
        ps = [group * DOWN_WIDTH + i for i in range(DOWN_WIDTH)]
        fields = [dot(remote_rows(p), parent_panel[p], NT).astype(jnp.bfloat16) for p in ps]
        totals = [leaf_sum[p] + dot(field, transfer[p], NN) for p, field in zip(ps, fields)]
        fars = []
        for p, total in zip(ps, totals):
            zero = jnp.zeros_like(total)
            stacked = jnp.concatenate(
                [jnp.where(low_lanes, total, zero), jnp.where(low_lanes, zero, total)], axis=0)
            weights = basis[pl.ds(2 * p, 2)].reshape(2 * rank, size)
            fars.append(dot(stacked.astype(jnp.bfloat16), weights, NN))
        for p, far in zip(ps, fars):
            out[2 * p] = (far[:rhs] + near_sum[2 * p]).astype(jnp.bfloat16)
            out[2 * p + 1] = (far[rhs:] + near_sum[2 * p + 1]).astype(jnp.bfloat16)

    for group in range(parents // DOWN_WIDTH):
        downward(group)
    for group, (index, condition) in tallies.items():
        rows = chunk * list(sends.values()).count(group)
        when(condition, moved(rows, send_sem.at[index], sibling_sem.at[0]).wait_send)


def on_device(
    streams,
    line,
    points_rhs,
    leaf_basis,
    transfer,
    leaf_coupling,
    parent_coupling,
    near_blocks,
    near_offsets,
    coupling_offsets,
    parent_owner,
    parent_local,
):
    leaves, rhs, size = points_rhs.shape
    parents, rank, _ = transfer.shape
    places = streams // 2
    nbits = bits_of(places)
    blocks = streams * line
    parts, near_parts = PARTS, 4
    hbm = pl.BlockSpec(memory_space=pltpu.HBM)
    bf16 = jnp.bfloat16
    dma = pltpu.SemaphoreType.DMA
    near_edge, far_edge = WIDTH + NEAR_REACH, WIDTH + FAR_REACH
    groups = parents // WIDTH
    offsets = [x.T for x in (near_offsets, coupling_offsets, parent_owner, parent_local)]
    return pl.pallas_call(
        functools.partial(kernel, streams, line, parts),
        out_shape=jax.ShapeDtypeStruct(points_rhs.shape, bf16),
        in_specs=[hbm] * 10,
        out_specs=pl.BlockSpec(memory_space=pltpu.VMEM),
        scratch_shapes=[
            *[pltpu.SMEM(x.shape, jnp.int32) for x in offsets],
            pltpu.VMEM(points_rhs.shape, bf16),
            pltpu.VMEM((near_edge + NEAR_REACH, rhs, size), bf16),
            pltpu.VMEM((near_edge + NEAR_REACH, rhs, size), bf16),
            pltpu.VMEM(leaf_basis.shape, bf16),
            pltpu.VMEM(transfer.shape, bf16),
            pltpu.VMEM(leaf_coupling.shape, bf16),
            pltpu.VMEM(parent_coupling.shape, bf16),
            pltpu.VMEM(near_blocks.shape, bf16),
            pltpu.VMEM((leaves, rhs, 2 * rank), bf16),
            pltpu.VMEM((far_edge + FAR_REACH, rhs, 2 * rank), bf16),
            pltpu.VMEM((far_edge + FAR_REACH, rhs, 2 * rank), bf16),
            pltpu.VMEM((blocks * parents, rhs // 2, 2 * rank), bf16),
            pltpu.VMEM((leaves, rhs, size), jnp.float32),
            pltpu.VMEM((parents, rhs, 2 * rank), jnp.float32),
            dma((4,)),
            dma((3 * groups,)),
            dma((2,)),
            dma((near_parts,)),
            dma((2,)),
            dma((4,)),
            dma((4,)),
            dma((line + 3 + sends_of(line, nbits) // blocks,)),
            dma((blocks // 2 * parts,)),
            dma((1,)),
            pltpu.SemaphoreType.REGULAR,
        ],
        compiler_params=pltpu.CompilerParams(
            collective_id=0, has_side_effects=True, vmem_limit_bytes=VMEM_LIMIT),
    )(
        *[pltpu.with_memory_space_constraint(x, pltpu.HBM) for x in (
            *offsets, points_rhs, leaf_basis, transfer, leaf_coupling, parent_coupling, near_blocks)]
    )


def solution(mesh):
    whole = P(("stream", "leaf"))
    return jax.shard_map(
        functools.partial(on_device, mesh.shape["stream"], mesh.shape["leaf"]),
        mesh=mesh,
        in_specs=(whole,) * 10,
        out_specs=whole,
        check_vma=False,
    )
```
